128 devices in a mesh: blk: 64 (over x, y_hi, z, core), rep: 2 (over y_lo).
Axes of the slice: x: 4, y: 4 (y_hi: 2, y_lo: 2; y = y_hi * 2 + y_lo), z: 4, core: 2. Of those that a mesh axis runs over, the one named last changes fastest.
Arguments:
- captions: bfloat16 [24576, 768], P(('blk', 'rep')), may hold values from -512 to 512
- images: bfloat16 [24576, 768], P(('blk', 'rep')), may hold values from -512 to 512
- positives: int32 [24576], P(('blk', 'rep')), may hold values from 0 to 24575, each once
- valid: int32 [24576], P(('blk', 'rep')), may hold values from 0 to 1, as said below
Outputs:
- caption_loss: float32 [24576], P(('blk', 'rep'))
- image_loss: float32 [24576], P(('blk', 'rep'))
- loss: float32 [], replicated
The draws below stay inside these ranges and needn't reach their ends.
Inputs may be any that keep to these rules, and one draw needn't show every extreme that they name: `positives`: each image row is the positive of exactly one caption; a program may pack several of these indices into one sent element. `valid`: the last image row is always real; a program may pack several of these flags into one sent element.
All inputs are finite; a program needn't handle non-finite values.
Results may differ from the reference program's by a relative error of at most 0.0003.
Values may be sent and summed in bfloat16 or wider, within the bound.
A program may use at most 128 MiB of HBM per device.

```python
import math
import jax
import jax.numpy as jnp
from jax import lax

E = 768
PAIRS = 24576


def pair_fields(key):
    base_key = jax.random.fold_in(key, 11)
    caption_key, image_key = jax.random.split(base_key, 2)
    caption_rows = jax.random.normal(caption_key, (PAIRS, E), jnp.float32)
    image_rows = jax.random.normal(image_key, (PAIRS, E), jnp.float32) * (3.0 / math.sqrt(E))
    return (caption_rows.astype(jnp.bfloat16), image_rows.astype(jnp.bfloat16))


def draw_captions(key, part):
    return pair_fields(key)[0]


def draw_images(key, part):
    return pair_fields(key)[1]


def draw_valid(key, part):
    position = jax.lax.iota(jnp.int32, PAIRS)
    rolled = jax.random.randint(jax.random.fold_in(key, 23), (PAIRS,), 0, 4 * PAIRS)
    flags = (rolled < PAIRS + 2 * position).astype(jnp.int32)
    return flags.at[PAIRS - 1].set(1)


def setup_inputs(seed: int = 0) -> dict:
    keys = jax.random.split(jax.random.key(seed), 5)
    captions = draw_captions(jax.random.fold_in(keys[4], 71), 0)
    images = draw_images(jax.random.fold_in(keys[4], 71), 0)
    positives = jax.random.permutation(keys[2], PAIRS).astype(jnp.int32)
    valid = draw_valid(jax.random.fold_in(keys[4], 71), 0)
    return {"captions": captions, "images": images, "positives": positives, "valid": valid}


very_low = -1.0e30


def reference(captions, images, positives, valid):
    pair_count = captions.shape[0]
    block_size = math.gcd(pair_count, 1024)
    image_ok = valid.astype(jnp.float32)
    caption_ok = jnp.take(image_ok, positives, axis=0)
    usable = image_ok[None, :] > 0
    columns = lax.iota(jnp.int32, pair_count)

    def one_block(running, block_index):
        column_peak, column_total, column_match = running
        offset = (block_index * block_size).astype(jnp.int32)
        caption_rows = lax.dynamic_slice_in_dim(captions, offset, block_size)
        match_rows = lax.dynamic_slice_in_dim(positives, offset, block_size)
        ok_rows = lax.dynamic_slice_in_dim(caption_ok, offset, block_size)
        scores = jnp.dot(caption_rows, images.T, preferred_element_type=jnp.float32)
        is_positive = match_rows[:, None] == columns[None, :]
        picked = jnp.where(is_positive, scores, 0.0)
        highest = jnp.max(jnp.where(usable, scores, very_low), axis=1)
        row_total = jnp.sum(jnp.where(usable, jnp.exp(scores - highest[:, None]), 0.0), axis=1)
        row_loss = ok_rows * (highest + jnp.log(row_total) - jnp.sum(picked, axis=1))
        caption_live = ok_rows[:, None] > 0
        column_high = jnp.max(jnp.where(caption_live, scores, very_low), axis=0)
        renewed = jnp.maximum(column_peak, column_high)
        powers = jnp.where(caption_live, jnp.exp(scores - renewed[None, :]), 0.0)
        column_total = column_total * jnp.exp(column_peak - renewed) + jnp.sum(powers, axis=0)
        column_match = column_match + jnp.sum(picked, axis=0)
        return (renewed, column_total, column_match), row_loss

    started = (jnp.full((pair_count,), very_low, jnp.float32), jnp.zeros((pair_count,), jnp.float32), jnp.zeros((pair_count,), jnp.float32))
    finished, row_losses = lax.scan(one_block, started, jnp.arange(pair_count // block_size, dtype=jnp.int32))
    caption_loss = row_losses.reshape(pair_count)
    image_loss = image_ok * (finished[0] + jnp.log(finished[1]) - finished[2])
    loss = (jnp.sum(caption_loss) + jnp.sum(image_loss)) / (2.0 * jnp.sum(image_ok))
    return (caption_loss, image_loss, loss)
```

```python
import functools

import jax
import jax.numpy as jnp
from jax import lax
from jax.experimental import pallas as pl
from jax.experimental.pallas import tpu as pltpu
from jax.sharding import Mesh
from jax.sharding import PartitionSpec as P

AXES = ("blk_0", "blk_1", "blk_2", "blk_3", "rep")
MESH = pl.DeviceIdType.MESH

ROWS = 192
PIECE = 64
WIDTH = 768
TILE = 2 * ROWS
BLOCK = 256
TILES = 8
BLOCKS = 6
LOW = -1e30
LOG2E = 1.4426950408889634
LN2 = 0.6931471805599453

FROM_LEFT = ((3, 0, 0), (3, 0, 1), (3, 0, 2), (2, 0, 0), (2, 0, 1), (3, 1, 2), (2, 1, 1))
FROM_RIGHT = ((1, 0, 0), (1, 0, 1), (1, 0, 2), (1, 1, 0), (2, 0, 2), (1, 1, 1), (2, 1, 0))
FROM_SIDE = ((0, 1, 0), (0, 1, 1), (0, 1, 2), (3, 1, 0), (3, 1, 1), (1, 1, 2), (2, 1, 2))
ARRIVALS = (FROM_LEFT, FROM_RIGHT, FROM_SIDE)
ROUNDS = 7
SLOT = {(0, 0, t): t for t in range(3)}
for _link, _list in enumerate(ARRIVALS):
    for _r, _chunk in enumerate(_list):
        SLOT[_chunk] = 3 * (_r + 1) + _link


def sent(link, r):
    d, s, t = ARRIVALS[link][r]
    if link == 0:
        return SLOT[((d + 1) % 4, s, t)]
    if link == 1:
        return SLOT[((d + 3) % 4, s, t)]
    return SLOT[(d, 1 - s, t)]


def release(link, r):
    return max(sent(link, k) // 3 for k in range(r + 1))


def items():
    done, order, starts, pairs = set(), [], {}, {}
    ready = (1, 2, 3, 5, 6, 7)
    for r in range(1, ROUNDS + 1):
        blocks = [b for b in range(BLOCKS) if ready[b] <= r]
        new = [b for b in blocks if ready[b] == r]
        first = [(p, b) for b in new for p in range(r)]
        later = [(r, b) for b in blocks]
        fresh = [i for i in first + later if i not in done]
        starts[r] = len(order)
        pairs[r] = len(order) + len([i for i in first if i not in done])
        order += fresh
        done |= set(fresh)
    return order, starts, pairs


ORDER, STARTS, PAIRS_AT = items()
ITEMS = len(ORDER)


def segments():
    found = []
    for i, (p, b) in enumerate(ORDER):
        if found:
            k, p0, b0, dp, db, n = found[-1]
            if n == 1:
                step = (p - p0, b - b0)
                if step in ((0, 1), (1, 0)):
                    found[-1] = (k, p0, b0, *step, 2)
                    continue
            elif (p0 + dp * n, b0 + db * n) == (p, b):
                found[-1] = (k, p0, b0, dp, db, n + 1)
                continue
        found.append((i, p, b, 0, 0, 1))
    return found


SEGMENTS = segments()


def place(i):
    tile, block = jnp.int32(0), jnp.int32(0)
    for k, p0, b0, dp, db, _ in SEGMENTS:
        tile = jnp.where(i >= k, p0 + dp * (i - k), tile)
        block = jnp.where(i >= k, b0 + db * (i - k), block)
    return tile, block


def row_place(slot, core):
    return (slot // 3) * TILE + core * ROWS + (slot % 3) * PIECE


def kernel(
    cap_in, img_in, pos_in, valid_in,
    cap_out, img_out, loss_out,
    cap, img, score0, score1, key, row_max, row_sum, row_match,
    col_max, col_sum, col_match, col_bias, col_id,
    meta, table, own_ok, row_msg, row_got, col_msg, col_got, part, part_got, part2, part2_got,
    load_sem, cap_send, cap_recv, img_send, img_recv, core_send, core_recv,
    meta_send, meta_recv, table_send, table_recv, row_send, row_recv, col_send, col_recv,
    a_send, a_recv, b_send, b_recv,
):
    x, yh, z, c, yl = (lax.axis_index(a) for a in AXES)

    def group_a(d, s, o):
        return (lax.rem(x + d, 4), yh, z, lax.rem(c + o, 2), lax.rem(yl + s, 2))

    def group_b(d, s):
        return (x, lax.rem(yh + s, 2), lax.rem(z + d, 4), c, lax.rem(yl + s, 2))

    members_a = [(d, s, o) for d in range(4) for s in range(2) for o in range(2) if (d, s, o) != (0, 0, 0)]
    members_b = [(d, s) for d in range(4) for s in range(2) if (d, s) != (0, 0)]

    def copy(src, dst, ssem, rsem, target):
        return pltpu.make_async_remote_copy(
            src_ref=src, dst_ref=dst, send_sem=ssem, recv_sem=rsem, device_id=target, device_id_type=MESH
        )

    def place_a(d, s, o):
        return (d * 2 + s) * 2 + o

    def place_b(d, s):
        return d * 2 + s

    load_cap = pltpu.make_async_copy(cap_in, cap.at[pl.ds(0, ROWS)], load_sem.at[0])
    load_img = pltpu.make_async_copy(img_in, img.at[pl.ds(0, ROWS)], load_sem.at[1])
    load_cap.start()
    load_img.start()

    barrier = pltpu.get_barrier_semaphore()
    for m in members_a:
        pl.semaphore_signal(barrier, inc=1, device_id=group_a(*m), device_id_type=MESH)
    for m in members_b:
        pl.semaphore_signal(barrier, inc=1, device_id=group_b(*m), device_id_type=MESH)

    lane = lax.broadcasted_iota(jnp.int32, (1, 128), 1)
    low_half = lane < 64
    pos_lo = pos_in[0:1, 0:128]
    pos_hi = jnp.concatenate([pos_in[0:1, 128:192], jnp.zeros((1, 64), jnp.int32)], axis=1)
    ok_lo = valid_in[0:1, 0:128]
    ok_hi = jnp.concatenate([valid_in[0:1, 128:192], jnp.zeros((1, 64), jnp.int32)], axis=1)
    meta[0, 0:1, :] = pos_lo + pos_hi * 32768
    meta[0, 1:2, :] = ok_lo + ok_hi * 2

    row_match[...] = jnp.zeros_like(row_match)
    col_max[...] = jnp.full_like(col_max, 2 * LOW)
    col_sum[...] = jnp.zeros_like(col_sum)
    col_match[...] = jnp.zeros_like(col_match)
    part[...] = jnp.zeros_like(part)

    pl.semaphore_wait(barrier, len(members_a) + len(members_b))

    meta_copies = {}
    for d, s, o in members_a:
        there = place_a((4 - d) % 4, s, o)
        meta_copies[(d, s, o)] = copy(
            meta.at[0], meta.at[there], meta_send.at[place_a(d, s, o)], meta_recv.at[there], group_a(d, s, o)
        )
        meta_copies[(d, s, o)].start()

    ring_a = (group_a(1, 0, 0), group_a(3, 0, 0), group_a(0, 1, 0))
    ring_b = (group_b(1, 0), group_b(3, 0), group_b(0, 1))
    other = group_a(0, 0, 1)

    def cap_copy(link, r):
        src, dst = row_place(sent(link, r), 0), row_place(3 * (r + 1) + link, 0)
        return copy(
            cap.at[pl.ds(src, PIECE)], cap.at[pl.ds(dst, PIECE)],
            cap_send.at[link * ROUNDS + r], cap_recv.at[link * ROUNDS + r], ring_a[link],
        )

    def img_copy(link, r):
        src, dst = sent(link, r) * PIECE, (3 * (r + 1) + link) * PIECE
        return copy(
            img.at[pl.ds(src, PIECE)], img.at[pl.ds(dst, PIECE)],
            img_send.at[link * ROUNDS + r], img_recv.at[link * ROUNDS + r], ring_b[link],
        )

    def core_copy(slot):
        return copy(
            cap.at[pl.ds(row_place(slot, 0), PIECE)], cap.at[pl.ds(row_place(slot, 1), PIECE)],
            core_send.at[slot], core_recv.at[slot], other,
        )

    def forward(after, which=(0, 1)):
        for r in range(ROUNDS):
            for link in range(3):
                if release(link, r) == after:
                    if 0 in which:
                        cap_copy(link, r).start()
                    if 1 in which:
                        img_copy(link, r).start()

    def arrive(r):
        for link in range(3):
            cap_copy(link, r - 1).wait_recv()
            core_copy(3 * r + link).start()
        for link in range(3):
            img_copy(link, r - 1).wait_recv()
        forward(r)

    def arrive_core(r):
        for link in range(3):
            core_copy(3 * r + link).wait_recv()

    load_cap.wait()
    load_img.wait()
    for r in range(2):
        for link in range(3):
            cap_copy(link, r).start()
            img_copy(link, r).start()
    for t in range(3):
        core_copy(t).start()

    for d, s, o in members_a:
        meta_copies[(d, s, o)].wait_recv()

    word = jnp.zeros((1, 128), jnp.int32)
    for d in range(4):
        for s in range(2):
            for o in range(2):
                at = lax.rem(x + d, 4) * 4 + lax.rem(c + o, 2) * 2 + lax.rem(yl + s, 2)
                word = word | lax.shift_left(
                    meta[place_a(d, s, o), 1:2, :], jnp.broadcast_to(2 * at, (1, 128))
                )
    mine = yh * 4 + z
    table[mine] = word
    table_copies = {}
    for d, s in members_b:
        table_copies[(d, s)] = copy(
            table.at[mine], table.at[mine], table_send.at[place_b(d, s)],
            table_recv.at[place_b((4 - d) % 4, s)], group_b(d, s),
        )
        table_copies[(d, s)].start()
    for link in range(3):
        cap_copy(link, 2).start()
        img_copy(link, 2).start()

    arrive(1)

    for d, s in members_b:
        there = lax.rem(yh + s, 2) * 4 + lax.rem(z + d, 4)
        copy(
            table.at[there], table.at[there], table_send.at[place_b(d, s)],
            table_recv.at[place_b(d, s)], group_b(d, s),
        ).wait_recv()

    for pair in range(12):
        ids, flags = [], []
        for half in range(2):
            slot = 2 * pair + half
            d, s, t = next(k for k, v in SLOT.items() if v == slot)
            ph, pz, pc = lax.rem(yh + s, 2), lax.rem(z + d, 4), lax.rem(yl + s, 2)
            device = (((x * 2 + ph) * 4 + pz) * 2 + c) * 2 + pc
            shift = 2 * (x * 4 + c * 2 + pc) + (1 if t == 2 else 0)
            bits = lax.shift_right_logical(table[ph * 4 + pz], jnp.broadcast_to(shift, (1, 128))) & 1
            if (t == 1) != (half == 1):
                bits = pltpu.roll(bits, 64, 1)
            flags.append(bits)
            ids.append(device * ROWS + t * PIECE - half * 64 + lane)
        flag = jnp.where(low_half, flags[0], flags[1])
        col_bias[0:1, pair * 128 : (pair + 1) * 128] = jnp.where(flag > 0, 0.0, LOW)
        col_id[0:1, pair * 128 : (pair + 1) * 128] = jnp.where(low_half, ids[0], ids[1]).astype(jnp.float32)

    words = jnp.concatenate([table[b] for b in range(8)], axis=0)
    bytes_ = jnp.concatenate(
        [(lax.shift_right_logical(words, jnp.full((8, 128), 8 * q, jnp.int32)) & 255) for q in range(4)], axis=0
    ).astype(jnp.float32).astype(jnp.bfloat16)
    sub = lax.broadcasted_iota(jnp.int32, (128, 128), 0)
    sub8 = lax.broadcasted_iota(jnp.int32, (8, 128), 0)

    def look_up(p):
        pick = ((p >> 6) * 171) >> 9
        row = p - pick * ROWS
        high = (row >= 128).astype(jnp.int32)
        at = row - 128 * high
        here = (((pick >> 4) & 1) << 2) + ((pick >> 2) & 3)
        bit = ((((pick >> 5) << 2) + (pick & 3)) << 1) + high
        hot = (sub == at).astype(jnp.float32).astype(jnp.bfloat16)
        got = jnp.dot(bytes_, hot, preferred_element_type=jnp.float32).astype(jnp.int32)
        value = jnp.zeros((1, 128), jnp.int32)
        for q in range(4):
            mine_q = jnp.sum(jnp.where(sub8 == here, got[8 * q : 8 * q + 8], 0), axis=0, keepdims=True)
            value = jnp.where((bit >> 3) == q, mine_q, value)
        return lax.shift_right_logical(value, bit & 7) & 1

    for d in range(4):
        for s in range(2):
            for o in range(2):
                packed = meta[place_a(d, s, o), 0:1, :]
                for half in range(2):
                    p = (packed & 32767) if half == 0 else (packed >> 15)
                    ok = look_up(p)
                    if (d, s, o) == (0, 0, 0):
                        own_ok[half : half + 1, :] = ok.astype(jnp.float32)
                    wanted = jnp.where(ok > 0, p, -1).astype(jnp.float32)
                    turned = jnp.transpose(jnp.broadcast_to(wanted, (128, 128)))
                    if half == 0:
                        key[pl.ds(row_place(SLOT[(d, s, 0)], o), PIECE)] = turned[:64]
                        key[pl.ds(row_place(SLOT[(d, s, 1)], o), PIECE)] = turned[64:]
                    else:
                        key[pl.ds(row_place(SLOT[(d, s, 2)], o), PIECE)] = turned[:64]

    for t in range(3):
        core_copy(t).wait_recv()
    arrive_core(1)

    scores = (score0, score1)

    def multiply(i, into):
        tile, block = place(i)
        rows = pl.ds(pl.multiple_of(tile * TILE, TILE), TILE)
        cols = pl.ds(pl.multiple_of(block * BLOCK, BLOCK), BLOCK)
        into[...] = lax.dot_general(
            cap[rows, :], img[cols, :], (((1,), (1,)), ((), ())), preferred_element_type=jnp.float32
        )

    def statistics(i, held):
        tile, block = place(i)
        first = pl.multiple_of(tile * TILE, TILE)
        cols = [pl.ds(pl.multiple_of(block * BLOCK, BLOCK) + 128 * h, 128) for h in range(2)]
        bias = [jnp.broadcast_to(col_bias[0:1, cols[h]], (PIECE, 128)) for h in range(2)]
        ids = [jnp.broadcast_to(col_id[0:1, cols[h]], (PIECE, 128)) for h in range(2)]
        before = [col_max[:, cols[h]] for h in range(2)]
        peak = list(before)
        for k in range(TILE // PIECE):
            rows = pl.ds(first + k * PIECE, PIECE)
            here = pl.ds(k * PIECE, PIECE)
            row_bias = jnp.where(key[rows, :] < 0, LOW, 0.0)
            values = []
            for h in range(2):
                u = held[here, 128 * h : 128 * h + 128] * LOG2E + bias[h] + row_bias
                held[here, 128 * h : 128 * h + 128] = u
                peak[h] = jnp.maximum(peak[h], jnp.max(u.reshape(PIECE // 8, 8, 128), axis=0))
                values.append(u)
            high = jnp.max(jnp.maximum(values[0], values[1]), axis=1, keepdims=True)
            row_max[block, rows, :] = jnp.broadcast_to(high, (PIECE, 128))
        total = [jnp.zeros((8, 128), jnp.float32) for _ in range(2)]
        match = [col_match[:, cols[h]] for h in range(2)]
        for k in range(TILE // PIECE):
            rows = pl.ds(first + k * PIECE, PIECE)
            here = pl.ds(k * PIECE, PIECE)
            high = row_max[block, rows, :]
            wanted = key[rows, :]
            found = row_match[rows, :]
            row_total = None
            for h in range(2):
                u = held[here, 128 * h : 128 * h + 128]
                e = jnp.exp2(u - high)
                row_total = e if row_total is None else row_total + e
                hit = wanted == ids[h]
                found = jnp.where(hit, u, found)
                for g in range(PIECE // 8):
                    part_u = u[8 * g : 8 * g + 8]
                    total[h] = total[h] + jnp.exp2(part_u - peak[h])
                    match[h] = jnp.where(hit[8 * g : 8 * g + 8], part_u, match[h])
            row_sum[block, rows, :] = row_total
            row_match[rows, :] = found
        for h in range(2):
            col_sum[:, cols[h]] = col_sum[:, cols[h]] * jnp.exp2(before[h] - peak[h]) + total[h]
            col_max[:, cols[h]] = peak[h]
            col_match[:, cols[h]] = match[h]

    multiply(jnp.int32(0), scores[0])

    @pl.loop(0, ITEMS // 2)
    def _(step):
        for half in range(2):
            i = step * 2 + half
            nxt = jnp.minimum(i + 1, ITEMS - 1)
            for r in range(2, ROUNDS + 1):
                if (STARTS[r] - 1) % 2 == half:
                    @pl.when(i + 1 == STARTS[r])
                    def _():
                        arrive(r)
                if (PAIRS_AT[r] - 1) % 2 == half:
                    @pl.when(i + 1 == PAIRS_AT[r])
                    def _():
                        arrive_core(r)
            multiply(nxt, scores[1 - half])
            statistics(i, scores[half])

    sub64 = lax.broadcasted_iota(jnp.int32, (PIECE, 128), 0)
    lane64 = lax.broadcasted_iota(jnp.int32, (PIECE, 128), 1)

    def row_result(slot, core, shift):
        rows = pl.ds(row_place(slot, core), PIECE)
        high = row_max[0, rows, :]
        for b in range(1, BLOCKS):
            high = jnp.maximum(high, row_max[b, rows, :])
        total = None
        for b in range(BLOCKS):
            term = row_sum[b, rows, :] * jnp.exp2(row_max[b, rows, :] - high)
            total = term if total is None else total + term
        lse = high + jnp.log2(jnp.sum(total, axis=1, keepdims=True))
        found = jnp.sum(row_match[rows, :], axis=1, keepdims=True)
        mine_lane = lane64 == sub64 + shift
        return (
            jnp.sum(jnp.where(mine_lane, lse, 0.0), axis=0, keepdims=True),
            jnp.sum(jnp.where(mine_lane, found, 0.0), axis=0, keepdims=True),
        )

    row_copies = []
    for d in range(4):
        for s in range(2):
            for o in range(2):
                at = place_a(d, s, o)
                first, second, third = (
                    row_result(SLOT[(d, s, t)], o, 64 if t == 1 else 0) for t in range(3)
                )
                into = row_got if at == 0 else row_msg
                into[at, 0:1, :] = first[0] + second[0]
                into[at, 1:2, :] = third[0]
                into[at, 2:3, :] = first[1] + second[1]
                into[at, 3:4, :] = third[1]
                if at:
                    there = place_a((4 - d) % 4, s, o)
                    out = copy(
                        row_msg.at[at], row_got.at[there], row_send.at[at], row_recv.at[there], group_a(d, s, o)
                    )
                    out.start()
                    row_copies.append(out)

    def merged(peak, total):
        high = jnp.max(peak, axis=0, keepdims=True)
        return high + jnp.log2(jnp.sum(total * jnp.exp2(peak - high), axis=0, keepdims=True))

    columns = []
    for pair in range(12):
        cols = pl.ds(pair * 128, 128)
        columns.append((
            merged(col_max[:, cols], col_sum[:, cols]),
            jnp.sum(col_match[:, cols], axis=0, keepdims=True),
        ))

    def third_of(slot, which, right):
        value = columns[slot // 2][which]
        return pltpu.roll(value, 64, 1) if (slot % 2 == 1) != right else value

    col_copies = []
    for d in range(4):
        for s in range(2):
            at = place_b(d, s)
            into = col_got if at == 0 else col_msg
            for which in range(2):
                left = third_of(SLOT[(d, s, 0)], which, False)
                right = third_of(SLOT[(d, s, 1)], which, True)
                into[at, 2 * which : 2 * which + 1, :] = jnp.where(low_half, left, right)
                into[at, 2 * which + 1 : 2 * which + 2, :] = third_of(SLOT[(d, s, 2)], which, False)
            if at:
                there = place_b((4 - d) % 4, s)
                out = copy(
                    col_msg.at[at], col_got.at[there], col_send.at[at], col_recv.at[there], group_b(d, s)
                )
                out.start()
                col_copies.append(out)

    for out in row_copies + col_copies:
        out.wait_recv()

    def joined(got):
        values = got[:, 0:2, :]
        high = jnp.max(values, axis=0)
        total = jnp.sum(jnp.exp2(values - high[None]), axis=0)
        return (high + jnp.log2(total) - jnp.sum(got[:, 2:4, :], axis=0)) * LN2

    usable = (lax.broadcasted_iota(jnp.int32, (2, 128), 0) == 0) | (
        lax.broadcasted_iota(jnp.int32, (2, 128), 1) < 64
    )
    cap_loss = jnp.where((own_ok[0:2, :] > 0) & usable, joined(row_got), 0.0)
    own_flags = jnp.concatenate([ok_lo, ok_hi], axis=0)
    img_loss = jnp.where((own_flags > 0) & usable, joined(col_got), 0.0)
    cap_out[0:1, 0:128] = cap_loss[0:1]
    cap_out[0:1, 128:192] = cap_loss[1:2, 0:64]
    img_out[0:1, 0:128] = img_loss[0:1]
    img_out[0:1, 128:192] = img_loss[1:2, 0:64]

    def spread(value, here, got, send, recv, members, index, target):
        here[0:1, :] = value
        outs = []
        for m in members:
            there = index((4 - m[0]) % 4, *m[1:])
            out = copy(here, got.at[there], send.at[index(*m)], recv.at[there], target(*m))
            out.start()
            outs.append(out)
        for out in outs:
            out.wait_recv()
        got[0] = here[...]
        return jnp.sum(got[...], axis=0)[0:1], outs

    both = cap_loss + img_loss
    total, outs_a = spread(
        both[0:1] + both[1:2], part, part_got, a_send, a_recv, members_a, place_a, group_a
    )
    part2[...] = jnp.zeros_like(part2)
    total, outs_b = spread(total, part2, part2_got, b_send, b_recv, members_b, place_b, group_b)
    count = jnp.zeros((8, 128), jnp.int32)
    for b in range(32):
        count = count + (lax.shift_right_logical(words, jnp.full((8, 128), b, jnp.int32)) & 1)
    real = jnp.sum(jnp.sum(count, axis=0, keepdims=True).astype(jnp.float32), axis=1, keepdims=True)
    loss_out[0:1, :] = jnp.broadcast_to(
        jnp.sum(total, axis=1, keepdims=True) / (2.0 * real), (1, 128)
    )

    for r in range(ROUNDS):
        for link in range(3):
            cap_copy(link, r).wait_send()
            img_copy(link, r).wait_send()
    for slot in range(24):
        core_copy(slot).wait_send()
    for out in [*meta_copies.values(), *table_copies.values(), *row_copies, *col_copies, *outs_a, *outs_b]:
        out.wait_send()


def local(captions, images, positives, valid):
    f32, i32 = jnp.float32, jnp.int32
    dma = pltpu.SemaphoreType.DMA
    vmem = pl.BlockSpec(memory_space=pltpu.VMEM)
    hbm = pl.BlockSpec(memory_space=pl.ANY)
    cap_loss, img_loss, loss = pl.pallas_call(
        kernel,
        out_shape=(
            jax.ShapeDtypeStruct((1, ROWS), f32),
            jax.ShapeDtypeStruct((1, ROWS), f32),
            jax.ShapeDtypeStruct((1, 128), f32),
        ),
        in_specs=[hbm, hbm, vmem, vmem],
        out_specs=(vmem, vmem, vmem),
        scratch_shapes=[
            pltpu.VMEM((TILES * TILE, WIDTH), jnp.bfloat16),
            pltpu.VMEM((BLOCKS * BLOCK, WIDTH), jnp.bfloat16),
            pltpu.VMEM((TILE, BLOCK), f32),
            pltpu.VMEM((TILE, BLOCK), f32),
            pltpu.VMEM((TILES * TILE, 128), f32),
            pltpu.VMEM((BLOCKS, TILES * TILE, 128), f32),
            pltpu.VMEM((BLOCKS, TILES * TILE, 128), f32),
            pltpu.VMEM((TILES * TILE, 128), f32),
            pltpu.VMEM((8, BLOCKS * BLOCK), f32),
            pltpu.VMEM((8, BLOCKS * BLOCK), f32),
            pltpu.VMEM((8, BLOCKS * BLOCK), f32),
            pltpu.VMEM((1, BLOCKS * BLOCK), f32),
            pltpu.VMEM((1, BLOCKS * BLOCK), f32),
            pltpu.VMEM((16, 2, 128), i32),
            pltpu.VMEM((8, 1, 128), i32),
            pltpu.VMEM((2, 128), f32),
            pltpu.VMEM((16, 4, 128), f32),
            pltpu.VMEM((16, 4, 128), f32),
            pltpu.VMEM((8, 4, 128), f32),
            pltpu.VMEM((8, 4, 128), f32),
            pltpu.VMEM((8, 128), f32),
            pltpu.VMEM((16, 8, 128), f32),
            pltpu.VMEM((8, 128), f32),
            pltpu.VMEM((8, 8, 128), f32),
            dma((2,)),
            dma((21,)), dma((21,)), dma((21,)), dma((21,)), dma((24,)), dma((24,)),
            dma((16,)), dma((16,)), dma((8,)), dma((8,)),
            dma((16,)), dma((16,)), dma((8,)), dma((8,)),
            dma((16,)), dma((16,)), dma((8,)), dma((8,)),
        ],
        compiler_params=pltpu.CompilerParams(
            collective_id=0, has_side_effects=True, vmem_limit_bytes=62 * 1024 * 1024
        ),
    )(captions, images, positives.reshape(1, ROWS), valid.reshape(1, ROWS))
    return cap_loss.reshape(ROWS), img_loss.reshape(ROWS), loss[0, 0]


def solution(mesh):
    torus = Mesh(mesh.devices.reshape(4, 2, 4, 2, mesh.shape["rep"]), AXES)
    return jax.shard_map(
        local,
        mesh=torus,
        in_specs=(P(AXES, None), P(AXES, None), P(AXES), P(AXES)),
        out_specs=(P(AXES), P(AXES), P()),
        check_vma=False,
    )
```

```python
import functools

import jax
import jax.numpy as jnp
from jax import lax
from jax.experimental import pallas as pl
from jax.experimental.pallas import tpu as pltpu
from jax.sharding import Mesh
from jax.sharding import PartitionSpec as P

AXES = ("blk_0", "blk_1", "blk_2", "blk_3", "rep")
MESH = pl.DeviceIdType.MESH

ROWS = 192
PIECE = 64
WIDTH = 768
TILE = 2 * ROWS
BLOCK = 256
TILES = 8
BLOCKS = 6
LOW = -1e30
LOG2E = 1.4426950408889634
LN2 = 0.6931471805599453

FROM_LEFT = ((3, 0, 0), (3, 0, 1), (3, 0, 2), (2, 0, 0), (2, 0, 1), (3, 1, 2), (2, 1, 1))
FROM_RIGHT = ((1, 0, 0), (1, 0, 1), (1, 0, 2), (1, 1, 0), (2, 0, 2), (1, 1, 1), (2, 1, 0))
FROM_SIDE = ((0, 1, 0), (0, 1, 1), (0, 1, 2), (3, 1, 0), (3, 1, 1), (1, 1, 2), (2, 1, 2))
ARRIVALS = (FROM_LEFT, FROM_RIGHT, FROM_SIDE)
ROUNDS = 7
SLOT = {(0, 0, t): t for t in range(3)}
for _link, _list in enumerate(ARRIVALS):
    for _r, _chunk in enumerate(_list):
        SLOT[_chunk] = 3 * (_r + 1) + _link


def sent(link, r):
    d, s, t = ARRIVALS[link][r]
    if link == 0:
        return SLOT[((d + 1) % 4, s, t)]
    if link == 1:
        return SLOT[((d + 3) % 4, s, t)]
    return SLOT[(d, 1 - s, t)]


def release(link, r):
    return max(sent(link, k) // 3 for k in range(r + 1))


def items():
    done, order, starts, pairs = set(), [], {}, {}
    ready = (1, 2, 3, 5, 6, 7)
    for r in range(1, ROUNDS + 1):
        blocks = [b for b in range(BLOCKS) if ready[b] <= r]
        new = [b for b in blocks if ready[b] == r]
        first = [(p, b) for b in new for p in range(r)]
        later = [(r, b) for b in blocks]
        fresh = [i for i in first + later if i not in done]
        starts[r] = len(order)
        pairs[r] = len(order) + len([i for i in first if i not in done])
        order += fresh
        done |= set(fresh)
    return order, starts, pairs


ORDER, STARTS, PAIRS_AT = items()
ITEMS = len(ORDER)
STEPS = ITEMS // 2
EARLY = 2
AT_STEP = {r: max(STARTS[r] // 2, 1) for r in STARTS}
CORE_AT_STEP = {r: max(PAIRS_AT[r] // 2, 1) for r in STARTS}


def segments():
    found = []
    for i, (p, b) in enumerate(ORDER):
        if found:
            k, p0, b0, dp, db, n = found[-1]
            if n == 1:
                step = (p - p0, b - b0)
                if step in ((0, 1), (1, 0)):
                    found[-1] = (k, p0, b0, *step, 2)
                    continue
            elif (p0 + dp * n, b0 + db * n) == (p, b):
                found[-1] = (k, p0, b0, dp, db, n + 1)
                continue
        found.append((i, p, b, 0, 0, 1))
    return found


SEGMENTS = segments()


def place(i):
    tile, block = jnp.int32(0), jnp.int32(0)
    for k, p0, b0, dp, db, _ in SEGMENTS:
        tile = jnp.where(i >= k, p0 + dp * (i - k), tile)
        block = jnp.where(i >= k, b0 + db * (i - k), block)
    return tile, block


def row_place(slot, core):
    return (slot // 3) * TILE + core * ROWS + (slot % 3) * PIECE


def kernel(
    cap_in, img_in, pos_in, valid_in,
    cap_out, img_out, loss_out,
    cap, img, score0, score1, score2, score3, key, row_bias, row_max, row_sum, row_match,
    col_max, col_sum, col_match, col_bias, col_id,
    meta, table, own_ok, row_msg, row_got, col_msg, col_got, part, part_got, part2, part2_got,
    load_sem, cap_send, cap_recv, img_send, img_recv, core_send, core_recv,
    meta_send, meta_recv, table_send, table_recv, row_send, row_recv, col_send, col_recv,
    a_send, a_recv, b_send, b_recv,
):
    x, yh, z, c, yl = (lax.axis_index(a) for a in AXES)
    scores = (score0, score1, score2, score3)

    def group_a(d, s, o):
        return (lax.rem(x + d, 4), yh, z, lax.rem(c + o, 2), lax.rem(yl + s, 2))

    def group_b(d, s):
        return (x, lax.rem(yh + s, 2), lax.rem(z + d, 4), c, lax.rem(yl + s, 2))

    members_a = [(d, s, o) for d in range(4) for s in range(2) for o in range(2) if (d, s, o) != (0, 0, 0)]
    members_b = [(d, s) for d in range(4) for s in range(2) if (d, s) != (0, 0)]

    def copy(src, dst, ssem, rsem, target):
        return pltpu.make_async_remote_copy(
            src_ref=src, dst_ref=dst, send_sem=ssem, recv_sem=rsem, device_id=target, device_id_type=MESH
        )

    def place_a(d, s, o):
        return (d * 2 + s) * 2 + o

    def place_b(d, s):
        return d * 2 + s

    load_cap = pltpu.make_async_copy(cap_in, cap.at[pl.ds(0, ROWS)], load_sem.at[0])
    load_img = pltpu.make_async_copy(img_in, img.at[pl.ds(0, ROWS)], load_sem.at[1])
    load_cap.start()
    load_img.start()

    barrier = pltpu.get_barrier_semaphore()
    for m in members_a:
        pl.semaphore_signal(barrier, inc=1, device_id=group_a(*m), device_id_type=MESH)
    for m in members_b:
        pl.semaphore_signal(barrier, inc=1, device_id=group_b(*m), device_id_type=MESH)

    lane = lax.broadcasted_iota(jnp.int32, (1, 128), 1)
    low_half = lane < 64
    pos_lo = pos_in[0:1, 0:128]
    pos_hi = jnp.concatenate([pos_in[0:1, 128:192], jnp.zeros((1, 64), jnp.int32)], axis=1)
    ok_lo = valid_in[0:1, 0:128]
    ok_hi = jnp.concatenate([valid_in[0:1, 128:192], jnp.zeros((1, 64), jnp.int32)], axis=1)
    meta[0, 0:1, :] = pos_lo + pos_hi * 32768
    meta[0, 1:2, :] = ok_lo + ok_hi * 2

    row_match[...] = jnp.zeros_like(row_match)
    part[...] = jnp.zeros_like(part)

    pl.semaphore_wait(barrier, len(members_a) + len(members_b))

    meta_copies = {}
    for d, s, o in members_a:
        there = place_a((4 - d) % 4, s, o)
        meta_copies[(d, s, o)] = copy(
            meta.at[0], meta.at[there], meta_send.at[place_a(d, s, o)], meta_recv.at[there], group_a(d, s, o)
        )
        meta_copies[(d, s, o)].start()

    ring_a = (group_a(1, 0, 0), group_a(3, 0, 0), group_a(0, 1, 0))
    ring_b = (group_b(1, 0), group_b(3, 0), group_b(0, 1))
    other = group_a(0, 0, 1)

    def cap_copy(link, r):
        src, dst = row_place(sent(link, r), 0), row_place(3 * (r + 1) + link, 0)
        return copy(
            cap.at[pl.ds(src, PIECE)], cap.at[pl.ds(dst, PIECE)],
            cap_send.at[link * ROUNDS + r], cap_recv.at[link * ROUNDS + r], ring_a[link],
        )

    def img_copy(link, r):
        src, dst = sent(link, r) * PIECE, (3 * (r + 1) + link) * PIECE
        return copy(
            img.at[pl.ds(src, PIECE)], img.at[pl.ds(dst, PIECE)],
            img_send.at[link * ROUNDS + r], img_recv.at[link * ROUNDS + r], ring_b[link],
        )

    def core_copy(slot):
        return copy(
            cap.at[pl.ds(row_place(slot, 0), PIECE)], cap.at[pl.ds(row_place(slot, 1), PIECE)],
            core_send.at[slot], core_recv.at[slot], other,
        )

    def forward(after, which=(0, 1)):
        for r in range(ROUNDS):
            for link in range(3):
                if release(link, r) == after:
                    if 0 in which:
                        cap_copy(link, r).start()
                    if 1 in which:
                        img_copy(link, r).start()

    def arrive(r):
        for link in range(3):
            cap_copy(link, r - 1).wait_recv()
            core_copy(3 * r + link).start()
        for link in range(3):
            img_copy(link, r - 1).wait_recv()
        forward(r)

    def arrive_core(r):
        for link in range(3):
            core_copy(3 * r + link).wait_recv()

    load_cap.wait()
    load_img.wait()
    for r in range(3):
        for link in range(3):
            cap_copy(link, r).start()
            if r == 0:
                img_copy(link, r).start()
    for t in range(3):
        core_copy(t).start()

    for d, s, o in members_a:
        meta_copies[(d, s, o)].wait_recv()

    word = jnp.zeros((1, 128), jnp.int32)
    for d in range(4):
        for s in range(2):
            for o in range(2):
                at = lax.rem(x + d, 4) * 4 + lax.rem(c + o, 2) * 2 + lax.rem(yl + s, 2)
                word = word | lax.shift_left(
                    meta[place_a(d, s, o), 1:2, :], jnp.broadcast_to(2 * at, (1, 128))
                )
    mine = yh * 4 + z
    table[mine] = word
    table_copies = {}
    for d, s in members_b:
        table_copies[(d, s)] = copy(
            table.at[mine], table.at[mine], table_send.at[place_b(d, s)],
            table_recv.at[place_b((4 - d) % 4, s)], group_b(d, s),
        )
        table_copies[(d, s)].start()
    for r in range(1, 3):
        for link in range(3):
            img_copy(link, r).start()

    for r in range(1, EARLY + 1):
        arrive(r)

    for d, s in members_b:
        there = lax.rem(yh + s, 2) * 4 + lax.rem(z + d, 4)
        copy(
            table.at[there], table.at[there], table_send.at[place_b(d, s)],
            table_recv.at[place_b(d, s)], group_b(d, s),
        ).wait_recv()

    for pair in range(12):
        ids, flags = [], []
        for half in range(2):
            slot = 2 * pair + half
            d, s, t = next(k for k, v in SLOT.items() if v == slot)
            ph, pz, pc = lax.rem(yh + s, 2), lax.rem(z + d, 4), lax.rem(yl + s, 2)
            device = (((x * 2 + ph) * 4 + pz) * 2 + c) * 2 + pc
            shift = 2 * (x * 4 + c * 2 + pc) + (1 if t == 2 else 0)
            bits = lax.shift_right_logical(table[ph * 4 + pz], jnp.broadcast_to(shift, (1, 128))) & 1
            if (t == 1) != (half == 1):
                bits = pltpu.roll(bits, 64, 1)
            flags.append(bits)
            ids.append(device * ROWS + t * PIECE - half * 64 + lane)
        flag = jnp.where(low_half, flags[0], flags[1])
        col_bias[0:1, pair * 128 : (pair + 1) * 128] = jnp.where(flag > 0, 0.0, LOW)
        col_id[0:1, pair * 128 : (pair + 1) * 128] = jnp.where(low_half, ids[0], ids[1]).astype(jnp.float32)

    words = jnp.concatenate([table[b] for b in range(8)], axis=0)
    bytes_ = jnp.concatenate(
        [(lax.shift_right_logical(words, jnp.full((8, 128), 8 * q, jnp.int32)) & 255) for q in range(4)], axis=0
    ).astype(jnp.float32).astype(jnp.bfloat16)
    sub = lax.broadcasted_iota(jnp.int32, (128, 128), 0)
    sub8 = lax.broadcasted_iota(jnp.int32, (8, 128), 0)

    def look_up(p):
        pick = ((p >> 6) * 171) >> 9
        row = p - pick * ROWS
        high = (row >= 128).astype(jnp.int32)
        at = row - 128 * high
        here = (((pick >> 4) & 1) << 2) + ((pick >> 2) & 3)
        bit = ((((pick >> 5) << 2) + (pick & 3)) << 1) + high
        hot = (sub == at).astype(jnp.float32).astype(jnp.bfloat16)
        got = jnp.dot(bytes_, hot, preferred_element_type=jnp.float32).astype(jnp.int32)
        value = jnp.zeros((1, 128), jnp.int32)
        for q in range(4):
            mine_q = jnp.sum(jnp.where(sub8 == here, got[8 * q : 8 * q + 8], 0), axis=0, keepdims=True)
            value = jnp.where((bit >> 3) == q, mine_q, value)
        return lax.shift_right_logical(value, bit & 7) & 1

    for d in range(4):
        for s in range(2):
            for o in range(2):
                packed = meta[place_a(d, s, o), 0:1, :]
                for half in range(2):
                    p = (packed & 32767) if half == 0 else (packed >> 15)
                    ok = look_up(p)
                    if (d, s, o) == (0, 0, 0):
                        own_ok[half : half + 1, :] = ok.astype(jnp.float32)
                    wanted = jnp.where(ok > 0, p, -1).astype(jnp.float32)
                    turned = jnp.transpose(jnp.broadcast_to(wanted, (128, 128)))
                    for t in (0, 1) if half == 0 else (2,):
                        rows = pl.ds(row_place(SLOT[(d, s, t)], o), PIECE)
                        value = turned[64 * (t % 2) : 64 * (t % 2) + 64]
                        key[rows, :] = value
                        row_bias[rows, :] = jnp.where(value < 0, LOW, 0.0)

    for t in range(3):
        core_copy(t).wait_recv()
    for r in range(1, EARLY + 1):
        arrive_core(r)

    def multiply(i, into):
        tile, block = place(i)
        rows = pl.ds(pl.multiple_of(tile * TILE, TILE), TILE)
        cols = pl.ds(pl.multiple_of(block * BLOCK, BLOCK), BLOCK)
        into[...] = lax.dot_general(
            cap[rows, :], img[cols, :], (((1,), (1,)), ((), ())), preferred_element_type=jnp.float32
        )

    def peaks(i, held):
        tile, block = place(i)
        first = pl.multiple_of(tile * TILE, TILE)
        cols = [pl.ds(pl.multiple_of(block * BLOCK, BLOCK) + 128 * h, 128) for h in range(2)]
        bias = [jnp.broadcast_to(col_bias[0:1, cols[h]], (PIECE, 128)) for h in range(2)]
        peak = [None, None]
        for k in range(TILE // PIECE):
            rows = pl.ds(first + k * PIECE, PIECE)
            here = pl.ds(k * PIECE, PIECE)
            low = row_bias[rows, :]
            values = []
            for h in range(2):
                u = held[here, 128 * h : 128 * h + 128] * LOG2E + bias[h] + low
                held[here, 128 * h : 128 * h + 128] = u
                top = jnp.max(u.reshape(PIECE // 8, 8, 128), axis=0)
                peak[h] = top if peak[h] is None else jnp.maximum(peak[h], top)
                values.append(u)
            high = jnp.max(jnp.maximum(values[0], values[1]), axis=1, keepdims=True)
            row_max[block, rows, :] = jnp.broadcast_to(high, (PIECE, 128))
        return peak

    def sums(i, held, peak):
        tile, block = place(i)
        first = pl.multiple_of(tile * TILE, TILE)
        cols = [pl.ds(pl.multiple_of(block * BLOCK, BLOCK) + 128 * h, 128) for h in range(2)]
        ids = [jnp.broadcast_to(col_id[0:1, cols[h]], (PIECE, 128)) for h in range(2)]
        total = [jnp.zeros((8, 128), jnp.float32) for _ in range(2)]
        match = [jnp.zeros((8, 128), jnp.float32) for _ in range(2)]
        for k in range(TILE // PIECE):
            rows = pl.ds(first + k * PIECE, PIECE)
            here = pl.ds(k * PIECE, PIECE)
            high = row_max[block, rows, :]
            wanted = key[rows, :]
            found = row_match[rows, :]
            row_total = None
            for h in range(2):
                u = held[here, 128 * h : 128 * h + 128]
                e = jnp.exp2(u - high)
                row_total = e if row_total is None else row_total + e
                hit = wanted == ids[h]
                found = jnp.where(hit, u, found)
                for g in range(PIECE // 8):
                    part_u = u[8 * g : 8 * g + 8]
                    total[h] = total[h] + jnp.exp2(part_u - peak[h])
                    match[h] = jnp.where(hit[8 * g : 8 * g + 8], part_u, match[h])
            row_sum[block, rows, :] = row_total
            row_match[rows, :] = found
        for h in range(2):
            col_max[tile, :, cols[h]] = peak[h]
            col_sum[tile, :, cols[h]] = total[h]
            col_match[tile, :, cols[h]] = match[h]

    multiply(jnp.int32(0), scores[0])
    multiply(jnp.int32(1), scores[1])

    @pl.loop(0, STEPS // 2)
    def _(turn):
        for half in range(2):
            step = turn * 2 + half
            for r in range(EARLY + 1, ROUNDS + 1):
                if (AT_STEP[r] - 1) % 2 == half:
                    @pl.when(step + 1 == AT_STEP[r])
                    def _():
                        arrive(r)
                if (CORE_AT_STEP[r] - 1) % 2 == half:
                    @pl.when(step + 1 == CORE_AT_STEP[r])
                    def _():
                        arrive_core(r)
            i = 2 * step
            nxt = jnp.minimum(i + 2, ITEMS - 2)
            now = scores[2 * half : 2 * half + 2]
            later = scores[2 - 2 * half : 4 - 2 * half]
            multiply(nxt, later[0])
            multiply(nxt + 1, later[1])
            tops = [peaks(i + k, now[k]) for k in range(2)]
            for k in range(2):
                sums(i + k, now[k], tops[k])

    sub64 = lax.broadcasted_iota(jnp.int32, (PIECE, 128), 0)
    lane64 = lax.broadcasted_iota(jnp.int32, (PIECE, 128), 1)

    def row_result(slot, core, shift):
        rows = pl.ds(row_place(slot, core), PIECE)
        high = row_max[0, rows, :]
        for b in range(1, BLOCKS):
            high = jnp.maximum(high, row_max[b, rows, :])
        total = None
        for b in range(BLOCKS):
            term = row_sum[b, rows, :] * jnp.exp2(row_max[b, rows, :] - high)
            total = term if total is None else total + term
        lse = high + jnp.log2(jnp.sum(total, axis=1, keepdims=True))
        found = jnp.sum(row_match[rows, :], axis=1, keepdims=True)
        mine_lane = lane64 == sub64 + shift
        return (
            jnp.sum(jnp.where(mine_lane, lse, 0.0), axis=0, keepdims=True),
            jnp.sum(jnp.where(mine_lane, found, 0.0), axis=0, keepdims=True),
        )

    row_copies = []
    for d in range(4):
        for s in range(2):
            for o in range(2):
                at = place_a(d, s, o)
                first, second, third = (
                    row_result(SLOT[(d, s, t)], o, 64 if t == 1 else 0) for t in range(3)
                )
                into = row_got if at == 0 else row_msg
                into[at, 0:1, :] = first[0] + second[0]
                into[at, 1:2, :] = third[0]
                into[at, 2:3, :] = first[1] + second[1]
                into[at, 3:4, :] = third[1]
                if at:
                    there = place_a((4 - d) % 4, s, o)
                    out = copy(
                        row_msg.at[at], row_got.at[there], row_send.at[at], row_recv.at[there], group_a(d, s, o)
                    )
                    out.start()
                    row_copies.append(out)

    def merged(peak, total):
        high = jnp.max(jnp.max(peak, axis=0), axis=0, keepdims=True)
        total = jnp.sum(total * jnp.exp2(peak - high[None]), axis=0)
        return high + jnp.log2(jnp.sum(total, axis=0, keepdims=True))

    columns = []
    for pair in range(12):
        cols = pl.ds(pair * 128, 128)
        columns.append((
            merged(col_max[:, :, cols], col_sum[:, :, cols]),
            jnp.sum(jnp.sum(col_match[:, :, cols], axis=0), axis=0, keepdims=True),
        ))

    def third_of(slot, which, right):
        value = columns[slot // 2][which]
        return pltpu.roll(value, 64, 1) if (slot % 2 == 1) != right else value

    col_copies = []
    for d in range(4):
        for s in range(2):
            at = place_b(d, s)
            into = col_got if at == 0 else col_msg
            for which in range(2):
                left = third_of(SLOT[(d, s, 0)], which, False)
                right = third_of(SLOT[(d, s, 1)], which, True)
                into[at, 2 * which : 2 * which + 1, :] = jnp.where(low_half, left, right)
                into[at, 2 * which + 1 : 2 * which + 2, :] = third_of(SLOT[(d, s, 2)], which, False)
            if at:
                there = place_b((4 - d) % 4, s)
                out = copy(
                    col_msg.at[at], col_got.at[there], col_send.at[at], col_recv.at[there], group_b(d, s)
                )
                out.start()
                col_copies.append(out)

    for out in row_copies + col_copies:
        out.wait_recv()

    def joined(got):
        values = got[:, 0:2, :]
        high = jnp.max(values, axis=0)
        total = jnp.sum(jnp.exp2(values - high[None]), axis=0)
        return (high + jnp.log2(total) - jnp.sum(got[:, 2:4, :], axis=0)) * LN2

    usable = (lax.broadcasted_iota(jnp.int32, (2, 128), 0) == 0) | (
        lax.broadcasted_iota(jnp.int32, (2, 128), 1) < 64
    )
    cap_loss = jnp.where((own_ok[0:2, :] > 0) & usable, joined(row_got), 0.0)
    own_flags = jnp.concatenate([ok_lo, ok_hi], axis=0)
    img_loss = jnp.where((own_flags > 0) & usable, joined(col_got), 0.0)
    cap_out[0:1, 0:128] = cap_loss[0:1]
    cap_out[0:1, 128:192] = cap_loss[1:2, 0:64]
    img_out[0:1, 0:128] = img_loss[0:1]
    img_out[0:1, 128:192] = img_loss[1:2, 0:64]

    def spread(value, here, got, send, recv, members, index, target):
        here[0:1, :] = value
        outs = []
        for m in members:
            there = index((4 - m[0]) % 4, *m[1:])
            out = copy(here, got.at[there], send.at[index(*m)], recv.at[there], target(*m))
            out.start()
            outs.append(out)
        for out in outs:
            out.wait_recv()
        got[0] = here[...]
        return jnp.sum(got[...], axis=0)[0:1], outs

    both = cap_loss + img_loss
    total, outs_a = spread(
        both[0:1] + both[1:2], part, part_got, a_send, a_recv, members_a, place_a, group_a
    )
    part2[...] = jnp.zeros_like(part2)
    total, outs_b = spread(total, part2, part2_got, b_send, b_recv, members_b, place_b, group_b)
    count = jnp.zeros((8, 128), jnp.int32)
    for b in range(32):
        count = count + (lax.shift_right_logical(words, jnp.full((8, 128), b, jnp.int32)) & 1)
    real = jnp.sum(jnp.sum(count, axis=0, keepdims=True).astype(jnp.float32), axis=1, keepdims=True)
    loss_out[0:1, :] = jnp.broadcast_to(
        jnp.sum(total, axis=1, keepdims=True) / (2.0 * real), (1, 128)
    )

    for r in range(ROUNDS):
        for link in range(3):
            cap_copy(link, r).wait_send()
            img_copy(link, r).wait_send()
    for slot in range(24):
        core_copy(slot).wait_send()
    for out in [*meta_copies.values(), *table_copies.values(), *row_copies, *col_copies, *outs_a, *outs_b]:
        out.wait_send()


def local(captions, images, positives, valid):
    f32, i32 = jnp.float32, jnp.int32
    dma = pltpu.SemaphoreType.DMA
    vmem = pl.BlockSpec(memory_space=pltpu.VMEM)
    hbm = pl.BlockSpec(memory_space=pl.ANY)
    cap_loss, img_loss, loss = pl.pallas_call(
        kernel,
        out_shape=(
            jax.ShapeDtypeStruct((1, ROWS), f32),
            jax.ShapeDtypeStruct((1, ROWS), f32),
            jax.ShapeDtypeStruct((1, 128), f32),
        ),
        in_specs=[hbm, hbm, vmem, vmem],
        out_specs=(vmem, vmem, vmem),
        scratch_shapes=[
            pltpu.VMEM((TILES * TILE, WIDTH), jnp.bfloat16),
            pltpu.VMEM((BLOCKS * BLOCK, WIDTH), jnp.bfloat16),
            *[pltpu.VMEM((TILE, BLOCK), f32)] * 4,
            pltpu.VMEM((TILES * TILE, 128), f32),
            pltpu.VMEM((TILES * TILE, 128), f32),
            pltpu.VMEM((BLOCKS, TILES * TILE, 128), f32),
            pltpu.VMEM((BLOCKS, TILES * TILE, 128), f32),
            pltpu.VMEM((TILES * TILE, 128), f32),
            pltpu.VMEM((TILES, 8, BLOCKS * BLOCK), f32),
            pltpu.VMEM((TILES, 8, BLOCKS * BLOCK), f32),
            pltpu.VMEM((TILES, 8, BLOCKS * BLOCK), f32),
            pltpu.VMEM((1, BLOCKS * BLOCK), f32),
            pltpu.VMEM((1, BLOCKS * BLOCK), f32),
            pltpu.VMEM((16, 2, 128), i32),
            pltpu.VMEM((8, 1, 128), i32),
            pltpu.VMEM((2, 128), f32),
            pltpu.VMEM((16, 4, 128), f32),
            pltpu.VMEM((16, 4, 128), f32),
            pltpu.VMEM((8, 4, 128), f32),
            pltpu.VMEM((8, 4, 128), f32),
            pltpu.VMEM((8, 128), f32),
            pltpu.VMEM((16, 8, 128), f32),
            pltpu.VMEM((8, 128), f32),
            pltpu.VMEM((8, 8, 128), f32),
            dma((2,)),
            dma((21,)), dma((21,)), dma((21,)), dma((21,)), dma((24,)), dma((24,)),
            dma((16,)), dma((16,)), dma((8,)), dma((8,)),
            dma((16,)), dma((16,)), dma((8,)), dma((8,)),
            dma((16,)), dma((16,)), dma((8,)), dma((8,)),
        ],
        compiler_params=pltpu.CompilerParams(
            collective_id=0, has_side_effects=True, vmem_limit_bytes=62 * 1024 * 1024
        ),
    )(captions, images, positives.reshape(1, ROWS), valid.reshape(1, ROWS))
    return cap_loss.reshape(ROWS), img_loss.reshape(ROWS), loss[0, 0]


def solution(mesh):
    torus = Mesh(mesh.devices.reshape(4, 2, 4, 2, mesh.shape["rep"]), AXES)
    return jax.shard_map(
        local,
        mesh=torus,
        in_specs=(P(AXES, None), P(AXES, None), P(AXES), P(AXES)),
        out_specs=(P(AXES), P(AXES), P()),
        check_vma=False,
    )
```

```python
import functools

import jax
import jax.numpy as jnp
from jax import lax
from jax.experimental import pallas as pl
from jax.experimental.pallas import tpu as pltpu
from jax.sharding import Mesh
from jax.sharding import PartitionSpec as P

AXES = ("blk_0", "blk_1", "blk_2", "blk_3", "rep")
MESH = pl.DeviceIdType.MESH

ROWS = 192
PIECE = 64
WIDTH = 768
TILE = 2 * ROWS
BLOCK = 256
TILES = 8
BLOCKS = 6
LOW = -1e30
LOG2E = 1.4426950408889634
LN2 = 0.6931471805599453

FROM_LEFT = ((3, 0, 0), (3, 0, 1), (3, 0, 2), (2, 0, 0), (2, 0, 1), (3, 1, 2), (2, 1, 1))
FROM_RIGHT = ((1, 0, 0), (1, 0, 1), (1, 0, 2), (1, 1, 0), (2, 0, 2), (1, 1, 1), (2, 1, 0))
FROM_SIDE = ((0, 1, 0), (0, 1, 1), (0, 1, 2), (3, 1, 0), (3, 1, 1), (1, 1, 2), (2, 1, 2))
ARRIVALS = (FROM_LEFT, FROM_RIGHT, FROM_SIDE)
ROUNDS = 7
SLOT = {(0, 0, t): t for t in range(3)}
for _link, _list in enumerate(ARRIVALS):
    for _r, _chunk in enumerate(_list):
        SLOT[_chunk] = 3 * (_r + 1) + _link


RIGHT = {k for (_, _, t), k in SLOT.items() if t == 1}


def sent(link, r):
    d, s, t = ARRIVALS[link][r]
    if link == 0:
        return SLOT[((d + 1) % 4, s, t)]
    if link == 1:
        return SLOT[((d + 3) % 4, s, t)]
    return SLOT[(d, 1 - s, t)]


def release(link, r):
    return max(sent(link, k) // 3 for k in range(r + 1))


def items():
    done, order, starts, pairs = set(), [], {}, {}
    ready = (1, 2, 3, 5, 6, 7)
    for r in range(1, ROUNDS + 1):
        blocks = [b for b in range(BLOCKS) if ready[b] <= r]
        new = [b for b in blocks if ready[b] == r]
        first = [(p, b) for b in new for p in range(r)]
        later = [(r, b) for b in blocks]
        fresh = [i for i in first + later if i not in done]
        starts[r] = len(order)
        pairs[r] = len(order) + len([i for i in first if i not in done])
        order += fresh
        done |= set(fresh)
    return order, starts, pairs


ORDER, STARTS, PAIRS_AT = items()
ITEMS = len(ORDER)
STEPS = ITEMS // 2
EARLY = 2
AT_STEP = {3: 1, 4: 4, 5: 7, 6: 11, 7: 16}
CORE_AT_STEP = {r: max(PAIRS_AT[r] // 2, 1) for r in STARTS}


def segments():
    found = []
    for i, (p, b) in enumerate(ORDER):
        if found:
            k, p0, b0, dp, db, n = found[-1]
            if n == 1:
                step = (p - p0, b - b0)
                if step in ((0, 1), (1, 0)):
                    found[-1] = (k, p0, b0, *step, 2)
                    continue
            elif (p0 + dp * n, b0 + db * n) == (p, b):
                found[-1] = (k, p0, b0, dp, db, n + 1)
                continue
        found.append((i, p, b, 0, 0, 1))
    return found


SEGMENTS = segments()


def place(i):
    tile, block = jnp.int32(0), jnp.int32(0)
    for k, p0, b0, dp, db, _ in SEGMENTS:
        tile = jnp.where(i >= k, p0 + dp * (i - k), tile)
        block = jnp.where(i >= k, b0 + db * (i - k), block)
    return tile, block


def row_place(slot, core):
    return (slot // 3) * TILE + core * ROWS + (slot % 3) * PIECE


def kernel(
    cap_in, img_in, pos_in, valid_in,
    cap_out, img_out, loss_out,
    cap, img, score0, score1, score2, score3, key, row_bias, row_max, row_sum, row_match,
    col_max, col_sum, col_match, col_bias, col_id,
    meta, table, cap_ok, img_ok, row_all, row_msg, row_got, row_lse, col_all, col_msg, col_got, col_lse,
    part_a, part_b,
    load_sem, cap_send, cap_recv, img_send, img_recv, core_send, core_recv,
    meta_send, meta_recv, table_send, table_recv, row_send, row_recv, col_send, col_recv,
    all_send, all_recv, call_send, call_recv,
    a_send, a_recv, b_send, b_recv,
):
    x, yh, z, c, yl = (lax.axis_index(a) for a in AXES)
    scores = (score0, score1, score2, score3)

    def group_a(d, s, o):
        return (lax.rem(x + d, 4), yh, z, lax.rem(c + o, 2), lax.rem(yl + s, 2))

    def group_b(d, s):
        return (x, lax.rem(yh + s, 2), lax.rem(z + d, 4), c, lax.rem(yl + s, 2))

    members_a = [(d, s, o) for d in range(4) for s in range(2) for o in range(2) if (d, s, o) != (0, 0, 0)]
    members_b = [(d, s) for d in range(4) for s in range(2) if (d, s) != (0, 0)]

    def copy(src, dst, ssem, rsem, target):
        return pltpu.make_async_remote_copy(
            src_ref=src, dst_ref=dst, send_sem=ssem, recv_sem=rsem, device_id=target, device_id_type=MESH
        )

    def place_a(d, s, o):
        return (d * 2 + s) * 2 + o

    def place_b(d, s):
        return d * 2 + s

    load_cap = pltpu.make_async_copy(cap_in, cap.at[pl.ds(0, ROWS)], load_sem.at[0])
    load_img = pltpu.make_async_copy(img_in, img.at[pl.ds(0, ROWS)], load_sem.at[1])
    load_cap.start()
    load_img.start()

    barrier = pltpu.get_barrier_semaphore()
    for m in members_a:
        pl.semaphore_signal(barrier, inc=1, device_id=group_a(*m), device_id_type=MESH)
    for m in members_b:
        pl.semaphore_signal(barrier, inc=1, device_id=group_b(*m), device_id_type=MESH)

    lane = lax.broadcasted_iota(jnp.int32, (1, 128), 1)
    low_half = lane < 64
    pos_lo = pos_in[0:1, 0:128]
    pos_hi = jnp.concatenate([pos_in[0:1, 128:192], jnp.zeros((1, 64), jnp.int32)], axis=1)
    ok_lo = valid_in[0:1, 0:128]
    ok_hi = jnp.concatenate([valid_in[0:1, 128:192], jnp.zeros((1, 64), jnp.int32)], axis=1)
    meta[0, 0:1, :] = pos_lo + pos_hi * 32768
    meta[0, 1:2, :] = ok_lo + ok_hi * 2

    row_match[...] = jnp.zeros_like(row_match)

    pl.semaphore_wait(barrier, len(members_a) + len(members_b))

    meta_copies = {}
    for d, s, o in members_a:
        there = place_a((4 - d) % 4, s, o)
        meta_copies[(d, s, o)] = copy(
            meta.at[0], meta.at[there], meta_send.at[place_a(d, s, o)], meta_recv.at[there], group_a(d, s, o)
        )
        meta_copies[(d, s, o)].start()

    ring_a = (group_a(1, 0, 0), group_a(3, 0, 0), group_a(0, 1, 0))
    ring_b = (group_b(1, 0), group_b(3, 0), group_b(0, 1))
    other = group_a(0, 0, 1)

    def cap_copy(link, r):
        src, dst = row_place(sent(link, r), 0), row_place(3 * (r + 1) + link, 0)
        return copy(
            cap.at[pl.ds(src, PIECE)], cap.at[pl.ds(dst, PIECE)],
            cap_send.at[link * ROUNDS + r], cap_recv.at[link * ROUNDS + r], ring_a[link],
        )

    def img_copy(link, r):
        src, dst = sent(link, r) * PIECE, (3 * (r + 1) + link) * PIECE
        return copy(
            img.at[pl.ds(src, PIECE)], img.at[pl.ds(dst, PIECE)],
            img_send.at[link * ROUNDS + r], img_recv.at[link * ROUNDS + r], ring_b[link],
        )

    def core_copy(slot):
        return copy(
            cap.at[pl.ds(row_place(slot, 0), PIECE)], cap.at[pl.ds(row_place(slot, 1), PIECE)],
            core_send.at[slot], core_recv.at[slot], other,
        )

    def forward(after, which=(0, 1)):
        for r in range(ROUNDS):
            for link in range(3):
                if release(link, r) == after:
                    if 0 in which:
                        cap_copy(link, r).start()
                    if 1 in which:
                        img_copy(link, r).start()

    def arrive(r):
        for link in range(3):
            cap_copy(link, r - 1).wait_recv()
            core_copy(3 * r + link).start()
        for link in range(3):
            img_copy(link, r - 1).wait_recv()
        forward(r)

    def arrive_core(r):
        for link in range(3):
            core_copy(3 * r + link).wait_recv()

    load_cap.wait()
    load_img.wait()
    for r in range(3):
        for link in range(3):
            cap_copy(link, r).start()
            if r < 2:
                img_copy(link, r).start()
    for t in range(3):
        core_copy(t).start()

    for d, s, o in members_a:
        meta_copies[(d, s, o)].wait_recv()

    word = jnp.zeros((1, 128), jnp.int32)
    for d in range(4):
        for s in range(2):
            for o in range(2):
                at = lax.rem(x + d, 4) * 4 + lax.rem(c + o, 2) * 2 + lax.rem(yl + s, 2)
                word = word | lax.shift_left(
                    meta[place_a(d, s, o), 1:2, :], jnp.broadcast_to(2 * at, (1, 128))
                )
    mine = yh * 4 + z
    table[mine] = word
    table_copies = {}
    for d, s in members_b:
        table_copies[(d, s)] = copy(
            table.at[mine], table.at[mine], table_send.at[place_b(d, s)],
            table_recv.at[place_b((4 - d) % 4, s)], group_b(d, s),
        )
        table_copies[(d, s)].start()
    for link in range(3):
        img_copy(link, 2).start()

    for r in range(1, EARLY + 1):
        arrive(r)

    for d, s in members_b:
        there = lax.rem(yh + s, 2) * 4 + lax.rem(z + d, 4)
        copy(
            table.at[there], table.at[there], table_send.at[place_b(d, s)],
            table_recv.at[place_b(d, s)], group_b(d, s),
        ).wait_recv()

    for d in range(4):
        for s in range(2):
            ph, pz, pc = lax.rem(yh + s, 2), lax.rem(z + d, 4), lax.rem(yl + s, 2)
            base = (pz * 2 + pc) * 2
            for half in range(2):
                shift = 2 * (x * 4 + c * 2 + pc) + half
                bits = lax.shift_right_logical(table[ph * 4 + pz], jnp.broadcast_to(shift, (1, 128))) & 1
                img_ok[pl.ds(base + half, 1), :] = bits.astype(jnp.float32)

    for pair in range(12):
        ids, flags = [], []
        for half in range(2):
            slot = 2 * pair + half
            d, s, t = next(k for k, v in SLOT.items() if v == slot)
            ph, pz, pc = lax.rem(yh + s, 2), lax.rem(z + d, 4), lax.rem(yl + s, 2)
            device = (((x * 2 + ph) * 4 + pz) * 2 + c) * 2 + pc
            shift = 2 * (x * 4 + c * 2 + pc) + (1 if t == 2 else 0)
            bits = lax.shift_right_logical(table[ph * 4 + pz], jnp.broadcast_to(shift, (1, 128))) & 1
            if (t == 1) != (half == 1):
                bits = pltpu.roll(bits, 64, 1)
            flags.append(bits)
            ids.append(device * ROWS + t * PIECE - half * 64 + lane)
        flag = jnp.where(low_half, flags[0], flags[1])
        col_bias[0:1, pair * 128 : (pair + 1) * 128] = jnp.where(flag > 0, 0.0, LOW)
        col_id[0:1, pair * 128 : (pair + 1) * 128] = jnp.where(low_half, ids[0], ids[1]).astype(jnp.float32)

    words = jnp.concatenate([table[b] for b in range(8)], axis=0)
    bytes_ = jnp.concatenate(
        [(lax.shift_right_logical(words, jnp.full((8, 128), 8 * q, jnp.int32)) & 255) for q in range(4)], axis=0
    ).astype(jnp.float32).astype(jnp.bfloat16)
    sub = lax.broadcasted_iota(jnp.int32, (128, 128), 0)
    sub8 = lax.broadcasted_iota(jnp.int32, (8, 128), 0)

    def look_up(p):
        pick = ((p >> 6) * 171) >> 9
        row = p - pick * ROWS
        high = (row >= 128).astype(jnp.int32)
        at = row - 128 * high
        here = (((pick >> 4) & 1) << 2) + ((pick >> 2) & 3)
        bit = ((((pick >> 5) << 2) + (pick & 3)) << 1) + high
        hot = (sub == at).astype(jnp.float32).astype(jnp.bfloat16)
        got = jnp.dot(bytes_, hot, preferred_element_type=jnp.float32).astype(jnp.int32)
        value = jnp.zeros((1, 128), jnp.int32)
        for q in range(4):
            mine_q = jnp.sum(jnp.where(sub8 == here, got[8 * q : 8 * q + 8], 0), axis=0, keepdims=True)
            value = jnp.where((bit >> 3) == q, mine_q, value)
        return lax.shift_right_logical(value, bit & 7) & 1

    for d in range(4):
        for s in range(2):
            base = (lax.rem(x + d, 4) * 2 + lax.rem(yl + s, 2)) * 3
            last = jnp.zeros((1, 128), jnp.float32)
            for o in range(2):
                packed = meta[place_a(d, s, o), 0:1, :]
                core = lax.rem(c + o, 2)
                for half in range(2):
                    p = (packed & 32767) if half == 0 else (packed >> 15)
                    ok = look_up(p)
                    real = ok.astype(jnp.float32)
                    if half == 0:
                        cap_ok[pl.ds(base + core, 1), :] = real
                    else:
                        real = jnp.where(low_half, real, 0.0)
                        last = last + jnp.where(core == 1, pltpu.roll(real, 64, 1), real)
                        if o == 1:
                            cap_ok[pl.ds(base + 2, 1), :] = last
                    wanted = jnp.where(ok > 0, p, -1).astype(jnp.float32)
                    turned = jnp.transpose(jnp.broadcast_to(wanted, (128, 128)))
                    for t in (0, 1) if half == 0 else (2,):
                        rows = pl.ds(row_place(SLOT[(d, s, t)], o), PIECE)
                        value = turned[64 * (t % 2) : 64 * (t % 2) + 64]
                        key[rows, :] = value
                        row_bias[rows, :] = jnp.where(value < 0, LOW, 0.0)

    for t in range(3):
        core_copy(t).wait_recv()
    for r in range(1, EARLY + 1):
        arrive_core(r)

    def multiply(i, into):
        tile, block = place(i)
        rows = pl.ds(pl.multiple_of(tile * TILE, TILE), TILE)
        cols = pl.ds(pl.multiple_of(block * BLOCK, BLOCK), BLOCK)
        into[...] = lax.dot_general(
            cap[rows, :], img[cols, :], (((1,), (1,)), ((), ())), preferred_element_type=jnp.float32
        )

    def peaks(i, held):
        tile, block = place(i)
        first = pl.multiple_of(tile * TILE, TILE)
        cols = [pl.ds(pl.multiple_of(block * BLOCK, BLOCK) + 128 * h, 128) for h in range(2)]
        bias = [jnp.broadcast_to(col_bias[0:1, cols[h]], (PIECE, 128)) for h in range(2)]
        peak = [None, None]
        for k in range(TILE // PIECE):
            rows = pl.ds(first + k * PIECE, PIECE)
            here = pl.ds(k * PIECE, PIECE)
            low = row_bias[rows, :]
            values = []
            for h in range(2):
                u = held[here, 128 * h : 128 * h + 128] * LOG2E + bias[h] + low
                held[here, 128 * h : 128 * h + 128] = u
                top = jnp.max(u.reshape(PIECE // 8, 8, 128), axis=0)
                peak[h] = top if peak[h] is None else jnp.maximum(peak[h], top)
                values.append(u)
            high = jnp.max(jnp.maximum(values[0], values[1]), axis=1, keepdims=True)
            row_max[block, rows, :] = jnp.broadcast_to(high, (PIECE, 128))
        return peak

    def sums(i, held, peak):
        tile, block = place(i)
        first = pl.multiple_of(tile * TILE, TILE)
        cols = [pl.ds(pl.multiple_of(block * BLOCK, BLOCK) + 128 * h, 128) for h in range(2)]
        ids = [jnp.broadcast_to(col_id[0:1, cols[h]], (PIECE, 128)) for h in range(2)]
        total = [jnp.zeros((8, 128), jnp.float32) for _ in range(2)]
        match = [jnp.zeros((8, 128), jnp.float32) for _ in range(2)]
        for k in range(TILE // PIECE):
            rows = pl.ds(first + k * PIECE, PIECE)
            here = pl.ds(k * PIECE, PIECE)
            high = row_max[block, rows, :]
            wanted = key[rows, :]
            found = row_match[rows, :]
            row_total = None
            for h in range(2):
                u = held[here, 128 * h : 128 * h + 128]
                e = jnp.exp2(u - high)
                row_total = e if row_total is None else row_total + e
                hit = wanted == ids[h]
                found = jnp.where(hit, u, found)
                for g in range(PIECE // 8):
                    part_u = u[8 * g : 8 * g + 8]
                    total[h] = total[h] + jnp.exp2(part_u - peak[h])
                    match[h] = jnp.where(hit[8 * g : 8 * g + 8], part_u, match[h])
            row_sum[block, rows, :] = row_total
            row_match[rows, :] = found
        for h in range(2):
            col_max[tile, :, cols[h]] = peak[h]
            col_sum[tile, :, cols[h]] = total[h]
            col_match[tile, :, cols[h]] = match[h]

    multiply(jnp.int32(0), scores[0])
    multiply(jnp.int32(1), scores[1])

    @pl.loop(0, STEPS // 2)
    def _(turn):
        for half in range(2):
            step = turn * 2 + half
            for r in range(EARLY + 1, ROUNDS + 1):
                if (AT_STEP[r] - 1) % 2 == half:
                    @pl.when(step + 1 == AT_STEP[r])
                    def _():
                        arrive(r)
                if (CORE_AT_STEP[r] - 1) % 2 == half:
                    @pl.when(step + 1 == CORE_AT_STEP[r])
                    def _():
                        arrive_core(r)
            i = 2 * step
            nxt = jnp.minimum(i + 2, ITEMS - 2)
            now = scores[2 * half : 2 * half + 2]
            later = scores[2 - 2 * half : 4 - 2 * half]
            multiply(nxt, later[0])
            multiply(nxt + 1, later[1])
            tops = [peaks(i + k, now[k]) for k in range(2)]
            for k in range(2):
                sums(i + k, now[k], tops[k])

    sub64 = lax.broadcasted_iota(jnp.int32, (PIECE, 128), 0)
    lane64 = lax.broadcasted_iota(jnp.int32, (PIECE, 128), 1)

    def row_result(slot, core, shift):
        rows = pl.ds(row_place(slot, core), PIECE)
        high = row_max[0, rows, :]
        for b in range(1, BLOCKS):
            high = jnp.maximum(high, row_max[b, rows, :])
        total = None
        for b in range(BLOCKS):
            term = row_sum[b, rows, :] * jnp.exp2(row_max[b, rows, :] - high)
            total = term if total is None else total + term
        lse = high + jnp.log2(jnp.sum(total, axis=1, keepdims=True))
        found = jnp.sum(row_match[rows, :], axis=1, keepdims=True)
        lse_lane = lane64 == sub64 + shift
        lane_shift = 64 if slot in RIGHT else 0
        found_lane = lane64 == sub64 + lane_shift
        return (
            jnp.sum(jnp.where(lse_lane, lse, 0.0), axis=0, keepdims=True),
            jnp.sum(jnp.where(found_lane, found, 0.0), axis=0, keepdims=True),
        )

    matched = jnp.zeros((1, 128), jnp.float32)
    for d in range(4):
        for s in range(2):
            base = (lax.rem(x + d, 4) * 2 + lax.rem(yl + s, 2)) * 3
            last = jnp.zeros((1, 128), jnp.float32)
            for o in range(2):
                at, core = place_a(d, s, o), lax.rem(c + o, 2)
                first, second = (row_result(SLOT[(d, s, t)], o, 64 * t) for t in range(2))
                third = row_result(SLOT[(d, s, 2)], o, 64 * core)
                row_all[0, pl.ds(base + core, 1), :] = first[0] + second[0]
                last = last + third[0]
                into = row_got if at == 0 else row_msg
                into[at, 0:1, :] = first[1] + second[1]
                into[at, 1:2, :] = third[1]
                matched = matched + first[1] + second[1] + third[1]
            row_all[0, pl.ds(base + 2, 1), :] = last
    row_got[0, 2:3, :] = matched
    for at in range(1, 16):
        row_msg[at, 2:3, :] = matched

    def merged(peak, total):
        high = jnp.max(jnp.max(peak, axis=0), axis=0, keepdims=True)
        total = jnp.sum(total * jnp.exp2(peak - high[None]), axis=0)
        return high + jnp.log2(jnp.sum(total, axis=0, keepdims=True))

    columns = []
    for pair in range(12):
        cols = pl.ds(pair * 128, 128)
        columns.append((
            merged(col_max[:, :, cols], col_sum[:, :, cols]),
            jnp.sum(jnp.sum(col_match[:, :, cols], axis=0), axis=0, keepdims=True),
        ))

    def third_of(slot, which, right):
        value = columns[slot // 2][which]
        return pltpu.roll(value, 64, 1) if (slot % 2 == 1) != right else value

    for d in range(4):
        for s in range(2):
            at = place_b(d, s)
            base = (lax.rem(z + d, 4) * 2 + lax.rem(yl + s, 2)) * 2
            into = col_got if at == 0 else col_msg
            for which in range(2):
                left = third_of(SLOT[(d, s, 0)], which, False)
                right = third_of(SLOT[(d, s, 1)], which, True)
                both = jnp.where(low_half, left, right)
                last = third_of(SLOT[(d, s, 2)], which, False)
                if which == 0:
                    col_all[0, pl.ds(base, 1), :] = both
                    col_all[0, pl.ds(base + 1, 1), :] = last
                else:
                    into[at, 0:1, :] = both
                    into[at, 1:2, :] = last

    def exchange(members, index, target, pairs):
        outs = []
        for m in members:
            here, there = index(*m), index((4 - m[0]) % 4, *m[1:])
            for src, dst, send, recv in pairs:
                outs.append(copy(
                    src(here), dst.at[there], send.at[here], recv.at[there], target(*m)
                ))
                outs[-1].start()
        return outs

    outs = exchange(members_a, place_a, group_a, [
        (lambda here: row_all.at[0], row_all, all_send, all_recv),
        (lambda here: row_msg.at[here], row_got, row_send, row_recv),
    ])
    outs += exchange(members_b, place_b, group_b, [
        (lambda here: col_all.at[0], col_all, call_send, call_recv),
        (lambda here: col_msg.at[here], col_got, col_send, col_recv),
    ])
    for out in outs:
        out.wait_recv()

    def joined(values):
        high = jnp.max(values, axis=0)
        return high + jnp.log2(jnp.sum(jnp.exp2(values - high[None]), axis=0))

    row_lse[...] = joined(row_all[...])
    col_lse[...] = joined(col_all[...])
    row_part = jnp.sum(jnp.where(cap_ok[...] > 0, row_lse[...], 0.0), axis=0, keepdims=True)
    found = jnp.sum(row_got[...], axis=0)
    part_b[0] = row_part - 2.0 * found[2:3]
    odd = lax.broadcasted_iota(jnp.int32, (16, 128), 0) & 1
    wide = lax.broadcasted_iota(jnp.int32, (16, 128), 1)
    counted = (img_ok[...] > 0) & ((odd == 0) | (wide < 64))
    part_a[0] = jnp.sum(jnp.where(counted, col_lse[...], 0.0), axis=0, keepdims=True)
    outs2 = exchange(members_a, place_a, group_a, [(lambda here: part_a.at[0], part_a, a_send, a_recv)])
    outs2 += exchange(members_b, place_b, group_b, [(lambda here: part_b.at[0], part_b, b_send, b_recv)])

    base = (x * 2 + yl) * 3
    cap_lo = row_lse[pl.ds(base + c, 1), :] - found[0:1]
    cap_hi = row_lse[pl.ds(base + 2, 1), :]
    cap_hi = jnp.where(c == 1, pltpu.roll(cap_hi, 64, 1), cap_hi) - found[1:2]
    real_hi = cap_ok[pl.ds(base + 2, 1), :]
    real_hi = jnp.where(c == 1, pltpu.roll(real_hi, 64, 1), real_hi)
    cap_out[0:1, 0:128] = jnp.where(cap_ok[pl.ds(base + c, 1), :] > 0, cap_lo * LN2, 0.0)
    cap_out[0:1, 128:192] = jnp.where(real_hi > 0, cap_hi * LN2, 0.0)[:, 0:64]
    base = (z * 2 + yl) * 2
    found = jnp.sum(col_got[...], axis=0)
    img_lo = col_lse[pl.ds(base, 1), :] - found[0:1]
    img_hi = col_lse[pl.ds(base + 1, 1), :] - found[1:2]
    img_out[0:1, 0:128] = jnp.where(ok_lo > 0, img_lo * LN2, 0.0)
    img_out[0:1, 128:192] = jnp.where(ok_hi > 0, img_hi * LN2, 0.0)[:, 0:64]
    count = jnp.zeros((8, 128), jnp.int32)
    for b in range(32):
        count = count + (lax.shift_right_logical(words, jnp.full((8, 128), b, jnp.int32)) & 1)
    real = jnp.sum(jnp.sum(count, axis=0, keepdims=True).astype(jnp.float32), axis=1, keepdims=True)

    for out in outs2:
        out.wait_recv()
    total = jnp.sum(part_a[...], axis=0) + jnp.sum(part_b[...], axis=0)
    loss_out[0:1, :] = jnp.broadcast_to(
        jnp.sum(total, axis=1, keepdims=True) * LN2 / (2.0 * real), (1, 128)
    )

    for r in range(ROUNDS):
        for link in range(3):
            cap_copy(link, r).wait_send()
            img_copy(link, r).wait_send()
    for slot in range(24):
        core_copy(slot).wait_send()
    for out in [*meta_copies.values(), *table_copies.values(), *outs, *outs2]:
        out.wait_send()


def local(captions, images, positives, valid):
    f32, i32 = jnp.float32, jnp.int32
    dma = pltpu.SemaphoreType.DMA
    vmem = pl.BlockSpec(memory_space=pltpu.VMEM)
    hbm = pl.BlockSpec(memory_space=pl.ANY)
    cap_loss, img_loss, loss = pl.pallas_call(
        kernel,
        out_shape=(
            jax.ShapeDtypeStruct((1, ROWS), f32),
            jax.ShapeDtypeStruct((1, ROWS), f32),
            jax.ShapeDtypeStruct((1, 128), f32),
        ),
        in_specs=[hbm, hbm, vmem, vmem],
        out_specs=(vmem, vmem, vmem),
        scratch_shapes=[
            pltpu.VMEM((TILES * TILE, WIDTH), jnp.bfloat16),
            pltpu.VMEM((BLOCKS * BLOCK, WIDTH), jnp.bfloat16),
            *[pltpu.VMEM((TILE, BLOCK), f32)] * 4,
            pltpu.VMEM((TILES * TILE, 128), f32),
            pltpu.VMEM((TILES * TILE, 128), f32),
            pltpu.VMEM((BLOCKS, TILES * TILE, 128), f32),
            pltpu.VMEM((BLOCKS, TILES * TILE, 128), f32),
            pltpu.VMEM((TILES * TILE, 128), f32),
            pltpu.VMEM((TILES, 8, BLOCKS * BLOCK), f32),
            pltpu.VMEM((TILES, 8, BLOCKS * BLOCK), f32),
            pltpu.VMEM((TILES, 8, BLOCKS * BLOCK), f32),
            pltpu.VMEM((1, BLOCKS * BLOCK), f32),
            pltpu.VMEM((1, BLOCKS * BLOCK), f32),
            pltpu.VMEM((16, 2, 128), i32),
            pltpu.VMEM((8, 1, 128), i32),
            pltpu.VMEM((24, 128), f32),
            pltpu.VMEM((16, 128), f32),
            pltpu.VMEM((16, 24, 128), f32),
            pltpu.VMEM((16, 3, 128), f32),
            pltpu.VMEM((16, 3, 128), f32),
            pltpu.VMEM((24, 128), f32),
            pltpu.VMEM((8, 16, 128), f32),
            pltpu.VMEM((8, 2, 128), f32),
            pltpu.VMEM((8, 2, 128), f32),
            pltpu.VMEM((16, 128), f32),
            pltpu.VMEM((16, 1, 128), f32),
            pltpu.VMEM((8, 1, 128), f32),
            dma((2,)),
            dma((21,)), dma((21,)), dma((21,)), dma((21,)), dma((24,)), dma((24,)),
            dma((16,)), dma((16,)), dma((8,)), dma((8,)),
            dma((16,)), dma((16,)), dma((8,)), dma((8,)),
            dma((16,)), dma((16,)), dma((8,)), dma((8,)),
            dma((16,)), dma((16,)), dma((8,)), dma((8,)),
        ],
        compiler_params=pltpu.CompilerParams(
            collective_id=0, has_side_effects=True, vmem_limit_bytes=62 * 1024 * 1024
        ),
    )(captions, images, positives.reshape(1, ROWS), valid.reshape(1, ROWS))
    return cap_loss.reshape(ROWS), img_loss.reshape(ROWS), loss[0, 0]


def solution(mesh):
    torus = Mesh(mesh.devices.reshape(4, 2, 4, 2, mesh.shape["rep"]), AXES)
    return jax.shard_map(
        local,
        mesh=torus,
        in_specs=(P(AXES, None), P(AXES, None), P(AXES), P(AXES)),
        out_specs=(P(AXES), P(AXES), P()),
        check_vma=False,
    )
```

```python
import functools

import jax
import jax.numpy as jnp
from jax import lax
from jax.experimental import pallas as pl
from jax.experimental.pallas import tpu as pltpu
from jax.sharding import Mesh
from jax.sharding import PartitionSpec as P

AXES = ("blk_0", "blk_1", "blk_2", "blk_3", "rep")
MESH = pl.DeviceIdType.MESH

ROWS = 192
PIECE = 64
WIDTH = 768
TILE = 2 * ROWS
BLOCK = 256
TILES = 8
BLOCKS = 6
LOW = -1e30
LOG2E = 1.4426950408889634
LN2 = 0.6931471805599453

FROM_LEFT = ((3, 0, 0), (3, 0, 1), (3, 0, 2), (2, 0, 0), (2, 0, 1), (3, 1, 2), (2, 1, 1))
FROM_RIGHT = ((1, 0, 0), (1, 0, 1), (1, 0, 2), (1, 1, 0), (2, 0, 2), (1, 1, 1), (2, 1, 0))
FROM_SIDE = ((0, 1, 0), (0, 1, 1), (0, 1, 2), (3, 1, 0), (3, 1, 1), (1, 1, 2), (2, 1, 2))
ARRIVALS = (FROM_LEFT, FROM_RIGHT, FROM_SIDE)
ROUNDS = 7
SLOT = {(0, 0, t): t for t in range(3)}
for _link, _list in enumerate(ARRIVALS):
    for _r, _chunk in enumerate(_list):
        SLOT[_chunk] = 3 * (_r + 1) + _link


RIGHT = {k for (_, _, t), k in SLOT.items() if t == 1}


def sent(link, r):
    d, s, t = ARRIVALS[link][r]
    if link == 0:
        return SLOT[((d + 1) % 4, s, t)]
    if link == 1:
        return SLOT[((d + 3) % 4, s, t)]
    return SLOT[(d, 1 - s, t)]


def release(link, r):
    return max(sent(link, k) // 3 for k in range(r + 1))


def items():
    done, order, starts, pairs = set(), [], {}, {}
    ready = (1, 2, 3, 5, 6, 7)
    for r in range(1, ROUNDS + 1):
        blocks = [b for b in range(BLOCKS) if ready[b] <= r]
        new = [b for b in blocks if ready[b] == r]
        first = [(p, b) for b in new for p in range(r)]
        later = [(r, b) for b in blocks]
        fresh = [i for i in first + later if i not in done]
        starts[r] = len(order)
        pairs[r] = len(order) + len([i for i in first if i not in done])
        order += fresh
        done |= set(fresh)
    return order, starts, pairs


ORDER, STARTS, PAIRS_AT = items()
ITEMS = len(ORDER)
STEPS = ITEMS // 2
EARLY = 2
AT_STEP = {3: 1, 4: 4, 5: 7, 6: 11, 7: 16}
CORE_AT_STEP = {r: max(PAIRS_AT[r] // 2, 1) for r in STARTS}


def segments():
    found = []
    for i, (p, b) in enumerate(ORDER):
        if found:
            k, p0, b0, dp, db, n = found[-1]
            if n == 1:
                step = (p - p0, b - b0)
                if step in ((0, 1), (1, 0)):
                    found[-1] = (k, p0, b0, *step, 2)
                    continue
            elif (p0 + dp * n, b0 + db * n) == (p, b):
                found[-1] = (k, p0, b0, dp, db, n + 1)
                continue
        found.append((i, p, b, 0, 0, 1))
    return found


SEGMENTS = segments()


def place(i):
    tile, block = jnp.int32(0), jnp.int32(0)
    for k, p0, b0, dp, db, _ in SEGMENTS:
        tile = jnp.where(i >= k, p0 + dp * (i - k), tile)
        block = jnp.where(i >= k, b0 + db * (i - k), block)
    return tile, block


def row_place(slot, core):
    return (slot // 3) * TILE + core * ROWS + (slot % 3) * PIECE


def kernel(
    cap_in, img_in, pos_in, valid_in,
    cap_out, img_out, loss_out,
    cap, img, score0, score1, score2, score3, key, row_bias, row_max, row_sum, row_match,
    col_max, col_sum, col_match, col_bias, col_id,
    meta, table, cap_ok, img_ok, row_all, row_msg, row_got, row_lse, col_all, col_msg, col_got, col_lse,
    part_a, part_b, cap_res, img_res,
    load_sem, out_sem, bulk_send, cap_recv, img_recv, core_recv, small_send, small_recv,
):
    x, yh, z, c, yl = (lax.axis_index(a) for a in AXES)
    scores = (score0, score1, score2, score3)

    def group_a(d, s, o):
        return (lax.rem(x + d, 4), yh, z, lax.rem(c + o, 2), lax.rem(yl + s, 2))

    def group_b(d, s):
        return (x, lax.rem(yh + s, 2), lax.rem(z + d, 4), c, lax.rem(yl + s, 2))

    members_a = [(d, s, o) for d in range(4) for s in range(2) for o in range(2) if (d, s, o) != (0, 0, 0)]
    members_b = [(d, s) for d in range(4) for s in range(2) if (d, s) != (0, 0)]

    def copy(src, dst, ssem, rsem, target):
        return pltpu.make_async_remote_copy(
            src_ref=src, dst_ref=dst, send_sem=ssem, recv_sem=rsem, device_id=target, device_id_type=MESH
        )

    def place_a(d, s, o):
        return (d * 2 + s) * 2 + o

    def place_b(d, s):
        return d * 2 + s

    load_cap = pltpu.make_async_copy(cap_in, cap.at[pl.ds(0, ROWS)], load_sem.at[0])
    load_img = pltpu.make_async_copy(img_in, img.at[pl.ds(0, ROWS)], load_sem.at[1])
    load_cap.start()
    load_img.start()

    barrier = pltpu.get_barrier_semaphore()
    for m in members_a:
        pl.semaphore_signal(barrier, inc=1, device_id=group_a(*m), device_id_type=MESH)
    for m in members_b:
        pl.semaphore_signal(barrier, inc=1, device_id=group_b(*m), device_id_type=MESH)

    lane = lax.broadcasted_iota(jnp.int32, (1, 128), 1)
    low_half = lane < 64
    pos_lo = pos_in[0:1, 0:128]
    pos_hi = jnp.concatenate([pos_in[0:1, 128:192], jnp.zeros((1, 64), jnp.int32)], axis=1)
    ok_lo = valid_in[0:1, 0:128]
    ok_hi = jnp.concatenate([valid_in[0:1, 128:192], jnp.zeros((1, 64), jnp.int32)], axis=1)
    meta[0, 0:1, :] = pos_lo + pos_hi * 32768
    meta[0, 1:2, :] = ok_lo + ok_hi * 2

    row_match[...] = jnp.zeros_like(row_match)

    pl.semaphore_wait(barrier, len(members_a) + len(members_b))

    for d, s, o in members_a:
        there = place_a((4 - d) % 4, s, o)
        copy(meta.at[0], meta.at[there], small_send.at[0], small_recv.at[0], group_a(d, s, o)).start()

    ring_a = (group_a(1, 0, 0), group_a(3, 0, 0), group_a(0, 1, 0))
    ring_b = (group_b(1, 0), group_b(3, 0), group_b(0, 1))
    other = group_a(0, 0, 1)

    def cap_copy(link, r):
        src, dst = row_place(sent(link, r), 0), row_place(3 * (r + 1) + link, 0)
        return copy(
            cap.at[pl.ds(src, PIECE)], cap.at[pl.ds(dst, PIECE)],
            bulk_send.at[0], cap_recv.at[r], ring_a[link],
        )

    def img_copy(link, r):
        src, dst = sent(link, r) * PIECE, (3 * (r + 1) + link) * PIECE
        return copy(
            img.at[pl.ds(src, PIECE)], img.at[pl.ds(dst, PIECE)],
            bulk_send.at[1], img_recv.at[r], ring_b[link],
        )

    def core_copy(r):
        return copy(
            cap.at[pl.ds(r * TILE, ROWS)], cap.at[pl.ds(r * TILE + ROWS, ROWS)],
            bulk_send.at[2], core_recv.at[r], other,
        )

    def all_of(ref, count, send, recv):
        part = ref.at[pl.ds(0, count)]
        return copy(part, part, send, recv, other)

    def forward(after, which=(0, 1)):
        for r in range(ROUNDS):
            for link in range(3):
                if release(link, r) == after:
                    if 0 in which:
                        cap_copy(link, r).start()
                    if 1 in which:
                        img_copy(link, r).start()

    def arrive(r):
        all_of(cap, ROWS, bulk_send.at[0], cap_recv.at[r - 1]).wait_recv()
        core_copy(r).start()
        all_of(img, ROWS, bulk_send.at[1], img_recv.at[r - 1]).wait_recv()
        forward(r)

    def arrive_core(r):
        core_copy(r).wait_recv()

    load_cap.wait()
    load_img.wait()
    for r in range(3):
        for link in range(3):
            cap_copy(link, r).start()
            if r < 2:
                img_copy(link, r).start()
    core_copy(0).start()

    all_of(meta, 15, small_send.at[0], small_recv.at[0]).wait_recv()

    word = jnp.zeros((1, 128), jnp.int32)
    for d in range(4):
        for s in range(2):
            for o in range(2):
                at = lax.rem(x + d, 4) * 4 + lax.rem(c + o, 2) * 2 + lax.rem(yl + s, 2)
                word = word | lax.shift_left(
                    meta[place_a(d, s, o), 1:2, :], jnp.broadcast_to(2 * at, (1, 128))
                )
    mine = yh * 4 + z
    table[mine] = word
    for d, s in members_b:
        copy(table.at[mine], table.at[mine], small_send.at[1], small_recv.at[1], group_b(d, s)).start()
    for link in range(3):
        img_copy(link, 2).start()

    for r in range(1, EARLY + 1):
        arrive(r)

    all_of(table, 7, small_send.at[1], small_recv.at[1]).wait_recv()

    for d in range(4):
        for s in range(2):
            ph, pz, pc = lax.rem(yh + s, 2), lax.rem(z + d, 4), lax.rem(yl + s, 2)
            base = (pz * 2 + pc) * 2
            for half in range(2):
                shift = 2 * (x * 4 + c * 2 + pc) + half
                bits = lax.shift_right_logical(table[ph * 4 + pz], jnp.broadcast_to(shift, (1, 128))) & 1
                img_ok[pl.ds(base + half, 1), :] = bits.astype(jnp.float32)

    for pair in range(12):
        ids, flags = [], []
        for half in range(2):
            slot = 2 * pair + half
            d, s, t = next(k for k, v in SLOT.items() if v == slot)
            ph, pz, pc = lax.rem(yh + s, 2), lax.rem(z + d, 4), lax.rem(yl + s, 2)
            device = (((x * 2 + ph) * 4 + pz) * 2 + c) * 2 + pc
            shift = 2 * (x * 4 + c * 2 + pc) + (1 if t == 2 else 0)
            bits = lax.shift_right_logical(table[ph * 4 + pz], jnp.broadcast_to(shift, (1, 128))) & 1
            if (t == 1) != (half == 1):
                bits = pltpu.roll(bits, 64, 1)
            flags.append(bits)
            ids.append(device * ROWS + t * PIECE - half * 64 + lane)
        flag = jnp.where(low_half, flags[0], flags[1])
        col_bias[0:1, pair * 128 : (pair + 1) * 128] = jnp.where(flag > 0, 0.0, LOW)
        col_id[0:1, pair * 128 : (pair + 1) * 128] = jnp.where(low_half, ids[0], ids[1]).astype(jnp.float32)

    words = jnp.concatenate([table[b] for b in range(8)], axis=0)
    bytes_ = jnp.concatenate(
        [(lax.shift_right_logical(words, jnp.full((8, 128), 8 * q, jnp.int32)) & 255) for q in range(4)], axis=0
    ).astype(jnp.float32).astype(jnp.bfloat16)
    sub = lax.broadcasted_iota(jnp.int32, (128, 128), 0)
    sub8 = lax.broadcasted_iota(jnp.int32, (8, 128), 0)

    def look_up(p):
        pick = ((p >> 6) * 171) >> 9
        row = p - pick * ROWS
        high = (row >= 128).astype(jnp.int32)
        at = row - 128 * high
        here = (((pick >> 4) & 1) << 2) + ((pick >> 2) & 3)
        bit = ((((pick >> 5) << 2) + (pick & 3)) << 1) + high
        hot = (sub == at).astype(jnp.float32).astype(jnp.bfloat16)
        got = jnp.dot(bytes_, hot, preferred_element_type=jnp.float32).astype(jnp.int32)
        value = jnp.zeros((1, 128), jnp.int32)
        for q in range(4):
            mine_q = jnp.sum(jnp.where(sub8 == here, got[8 * q : 8 * q + 8], 0), axis=0, keepdims=True)
            value = jnp.where((bit >> 3) == q, mine_q, value)
        return lax.shift_right_logical(value, bit & 7) & 1

    for d in range(4):
        for s in range(2):
            base = (lax.rem(x + d, 4) * 2 + lax.rem(yl + s, 2)) * 3
            last = jnp.zeros((1, 128), jnp.float32)
            for o in range(2):
                packed = meta[place_a(d, s, o), 0:1, :]
                core = lax.rem(c + o, 2)
                for half in range(2):
                    p = (packed & 32767) if half == 0 else (packed >> 15)
                    ok = look_up(p)
                    real = ok.astype(jnp.float32)
                    if half == 0:
                        cap_ok[pl.ds(base + core, 1), :] = real
                    else:
                        real = jnp.where(low_half, real, 0.0)
                        last = last + jnp.where(core == 1, pltpu.roll(real, 64, 1), real)
                        if o == 1:
                            cap_ok[pl.ds(base + 2, 1), :] = last
                    wanted = jnp.where(ok > 0, p, -1).astype(jnp.float32)
                    turned = jnp.transpose(jnp.broadcast_to(wanted, (128, 128)))
                    for t in (0, 1) if half == 0 else (2,):
                        rows = pl.ds(row_place(SLOT[(d, s, t)], o), PIECE)
                        value = turned[64 * (t % 2) : 64 * (t % 2) + 64]
                        key[rows, :] = value
                        row_bias[rows, :] = jnp.where(value < 0, LOW, 0.0)

    for r in range(EARLY + 1):
        arrive_core(r)

    def multiply(i, into):
        tile, block = place(i)
        rows = pl.ds(pl.multiple_of(tile * TILE, TILE), TILE)
        cols = pl.ds(pl.multiple_of(block * BLOCK, BLOCK), BLOCK)
        into[...] = lax.dot_general(
            cap[rows, :], img[cols, :], (((1,), (1,)), ((), ())), preferred_element_type=jnp.float32
        )

    def peaks(i, held):
        tile, block = place(i)
        first = pl.multiple_of(tile * TILE, TILE)
        cols = [pl.ds(pl.multiple_of(block * BLOCK, BLOCK) + 128 * h, 128) for h in range(2)]
        bias = [jnp.broadcast_to(col_bias[0:1, cols[h]], (PIECE, 128)) for h in range(2)]
        peak = [None, None]
        for k in range(TILE // PIECE):
            rows = pl.ds(first + k * PIECE, PIECE)
            here = pl.ds(k * PIECE, PIECE)
            low = row_bias[rows, :]
            values = []
            for h in range(2):
                u = held[here, 128 * h : 128 * h + 128] * LOG2E + bias[h] + low
                held[here, 128 * h : 128 * h + 128] = u
                top = jnp.max(u.reshape(PIECE // 8, 8, 128), axis=0)
                peak[h] = top if peak[h] is None else jnp.maximum(peak[h], top)
                values.append(u)
            high = jnp.max(jnp.maximum(values[0], values[1]), axis=1, keepdims=True)
            row_max[block, rows, :] = jnp.broadcast_to(high, (PIECE, 128))
        return peak

    def sums(i, held, peak):
        tile, block = place(i)
        first = pl.multiple_of(tile * TILE, TILE)
        cols = [pl.ds(pl.multiple_of(block * BLOCK, BLOCK) + 128 * h, 128) for h in range(2)]
        ids = [jnp.broadcast_to(col_id[0:1, cols[h]], (PIECE, 128)) for h in range(2)]
        total = [jnp.zeros((8, 128), jnp.float32) for _ in range(2)]
        match = [jnp.zeros((8, 128), jnp.float32) for _ in range(2)]
        for k in range(TILE // PIECE):
            rows = pl.ds(first + k * PIECE, PIECE)
            here = pl.ds(k * PIECE, PIECE)
            high = row_max[block, rows, :]
            wanted = key[rows, :]
            found = row_match[rows, :]
            row_total = None
            for h in range(2):
                u = held[here, 128 * h : 128 * h + 128]
                e = jnp.exp2(u - high)
                row_total = e if row_total is None else row_total + e
                hit = wanted == ids[h]
                found = jnp.where(hit, u, found)
                for g in range(PIECE // 8):
                    part_u = u[8 * g : 8 * g + 8]
                    total[h] = total[h] + jnp.exp2(part_u - peak[h])
                    match[h] = jnp.where(hit[8 * g : 8 * g + 8], part_u, match[h])
            row_sum[block, rows, :] = row_total
            row_match[rows, :] = found
        for h in range(2):
            col_max[tile, :, cols[h]] = peak[h]
            col_sum[tile, :, cols[h]] = total[h]
            col_match[tile, :, cols[h]] = match[h]

    multiply(jnp.int32(0), scores[0])
    multiply(jnp.int32(1), scores[1])

    @pl.loop(0, STEPS // 2)
    def _(turn):
        for half in range(2):
            step = turn * 2 + half
            for r in range(EARLY + 1, ROUNDS + 1):
                if (AT_STEP[r] - 1) % 2 == half:
                    @pl.when(step + 1 == AT_STEP[r])
                    def _():
                        arrive(r)
                if (CORE_AT_STEP[r] - 1) % 2 == half:
                    @pl.when(step + 1 == CORE_AT_STEP[r])
                    def _():
                        arrive_core(r)
            i = 2 * step
            nxt = jnp.minimum(i + 2, ITEMS - 2)
            now = scores[2 * half : 2 * half + 2]
            later = scores[2 - 2 * half : 4 - 2 * half]
            multiply(nxt, later[0])
            multiply(nxt + 1, later[1])
            tops = [peaks(i + k, now[k]) for k in range(2)]
            for k in range(2):
                sums(i + k, now[k], tops[k])

    sub64 = lax.broadcasted_iota(jnp.int32, (PIECE, 128), 0)
    lane64 = lax.broadcasted_iota(jnp.int32, (PIECE, 128), 1)

    def row_result(slot, core, shift):
        rows = pl.ds(row_place(slot, core), PIECE)
        high = row_max[0, rows, :]
        for b in range(1, BLOCKS):
            high = jnp.maximum(high, row_max[b, rows, :])
        total = None
        for b in range(BLOCKS):
            term = row_sum[b, rows, :] * jnp.exp2(row_max[b, rows, :] - high)
            total = term if total is None else total + term
        lse = high + jnp.log2(jnp.sum(total, axis=1, keepdims=True))
        found = jnp.sum(row_match[rows, :], axis=1, keepdims=True)
        lse_lane = lane64 == sub64 + shift
        lane_shift = 64 if slot in RIGHT else 0
        found_lane = lane64 == sub64 + lane_shift
        return (
            jnp.sum(jnp.where(lse_lane, lse, 0.0), axis=0, keepdims=True),
            jnp.sum(jnp.where(found_lane, found, 0.0), axis=0, keepdims=True),
        )

    matched = jnp.zeros((1, 128), jnp.float32)
    for d in range(4):
        for s in range(2):
            base = (lax.rem(x + d, 4) * 2 + lax.rem(yl + s, 2)) * 3
            last = jnp.zeros((1, 128), jnp.float32)
            for o in range(2):
                at, core = place_a(d, s, o), lax.rem(c + o, 2)
                first, second = (row_result(SLOT[(d, s, t)], o, 64 * t) for t in range(2))
                third = row_result(SLOT[(d, s, 2)], o, 64 * core)
                row_all[0, pl.ds(base + core, 1), :] = first[0] + second[0]
                last = last + third[0]
                into = row_got if at == 0 else row_msg
                into[at, 0:1, :] = first[1] + second[1]
                into[at, 1:2, :] = third[1]
                matched = matched + first[1] + second[1] + third[1]
            row_all[0, pl.ds(base + 2, 1), :] = last
    row_got[0, 2:3, :] = matched
    for at in range(1, 16):
        row_msg[at, 2:3, :] = matched

    def merged(peak, total):
        high = jnp.max(jnp.max(peak, axis=0), axis=0, keepdims=True)
        total = jnp.sum(total * jnp.exp2(peak - high[None]), axis=0)
        return high + jnp.log2(jnp.sum(total, axis=0, keepdims=True))

    columns = []
    for pair in range(12):
        cols = pl.ds(pair * 128, 128)
        columns.append((
            merged(col_max[:, :, cols], col_sum[:, :, cols]),
            jnp.sum(jnp.sum(col_match[:, :, cols], axis=0), axis=0, keepdims=True),
        ))

    def third_of(slot, which, right):
        value = columns[slot // 2][which]
        return pltpu.roll(value, 64, 1) if (slot % 2 == 1) != right else value

    for d in range(4):
        for s in range(2):
            at = place_b(d, s)
            base = (lax.rem(z + d, 4) * 2 + lax.rem(yl + s, 2)) * 2
            into = col_got if at == 0 else col_msg
            for which in range(2):
                left = third_of(SLOT[(d, s, 0)], which, False)
                right = third_of(SLOT[(d, s, 1)], which, True)
                both = jnp.where(low_half, left, right)
                last = third_of(SLOT[(d, s, 2)], which, False)
                if which == 0:
                    col_all[0, pl.ds(base, 1), :] = both
                    col_all[0, pl.ds(base + 1, 1), :] = last
                else:
                    into[at, 0:1, :] = both
                    into[at, 1:2, :] = last

    def exchange(members, index, target, pairs):
        for m in members:
            here, there = index(*m), index((4 - m[0]) % 4, *m[1:])
            for src, dst, k in pairs:
                copy(src(here), dst.at[there], small_send.at[k], small_recv.at[k], target(*m)).start()

    def exchanged(refs):
        return [all_of(ref, count, small_send.at[k], small_recv.at[k]) for ref, count, k in refs]

    exchange(members_a, place_a, group_a, [
        (lambda here: row_all.at[0], row_all, 2), (lambda here: row_msg.at[here], row_got, 3),
    ])
    exchange(members_b, place_b, group_b, [
        (lambda here: col_all.at[0], col_all, 4), (lambda here: col_msg.at[here], col_got, 5),
    ])
    outs = exchanged([(row_all, 15, 2), (row_got, 15, 3), (col_all, 7, 4), (col_got, 7, 5)])
    for out in outs:
        out.wait_recv()

    def joined(values):
        high = jnp.max(values, axis=0)
        return high + jnp.log2(jnp.sum(jnp.exp2(values - high[None]), axis=0))

    row_lse[...] = joined(row_all[...])
    col_lse[...] = joined(col_all[...])
    row_part = jnp.sum(jnp.where(cap_ok[...] > 0, row_lse[...], 0.0), axis=0, keepdims=True)
    found = jnp.sum(row_got[...], axis=0)
    part_b[0] = row_part - 2.0 * found[2:3]
    odd = lax.broadcasted_iota(jnp.int32, (16, 128), 0) & 1
    wide = lax.broadcasted_iota(jnp.int32, (16, 128), 1)
    counted = (img_ok[...] > 0) & ((odd == 0) | (wide < 64))
    part_a[0] = jnp.sum(jnp.where(counted, col_lse[...], 0.0), axis=0, keepdims=True)
    exchange(members_a, place_a, group_a, [(lambda here: part_a.at[0], part_a, 6)])
    exchange(members_b, place_b, group_b, [(lambda here: part_b.at[0], part_b, 7)])
    outs2 = exchanged([(part_a, 15, 6), (part_b, 7, 7)])

    base = (x * 2 + yl) * 3
    cap_lo = row_lse[pl.ds(base + c, 1), :] - found[0:1]
    cap_hi = row_lse[pl.ds(base + 2, 1), :]
    cap_hi = jnp.where(c == 1, pltpu.roll(cap_hi, 64, 1), cap_hi) - found[1:2]
    real_hi = cap_ok[pl.ds(base + 2, 1), :]
    real_hi = jnp.where(c == 1, pltpu.roll(real_hi, 64, 1), real_hi)
    cap_res[0:128] = jnp.where(cap_ok[pl.ds(base + c, 1), :] > 0, cap_lo * LN2, 0.0).reshape(128)
    cap_res[128:192] = jnp.where(real_hi > 0, cap_hi * LN2, 0.0)[:, 0:64].reshape(64)
    base = (z * 2 + yl) * 2
    found = jnp.sum(col_got[...], axis=0)
    img_lo = col_lse[pl.ds(base, 1), :] - found[0:1]
    img_hi = col_lse[pl.ds(base + 1, 1), :] - found[1:2]
    img_res[0:128] = jnp.where(ok_lo > 0, img_lo * LN2, 0.0).reshape(128)
    img_res[128:192] = jnp.where(ok_hi > 0, img_hi * LN2, 0.0)[:, 0:64].reshape(64)
    results = [
        pltpu.make_async_copy(cap_res, cap_out, out_sem.at[0]), pltpu.make_async_copy(img_res, img_out, out_sem.at[1])
    ]
    for result in results:
        result.start()
    count = jnp.zeros((8, 128), jnp.int32)
    for b in range(32):
        count = count + (lax.shift_right_logical(words, jnp.full((8, 128), b, jnp.int32)) & 1)
    real = jnp.sum(jnp.sum(count, axis=0, keepdims=True).astype(jnp.float32), axis=1, keepdims=True)

    all_of(cap, 3 * ROUNDS * PIECE, bulk_send.at[0], cap_recv.at[0]).wait_send()
    all_of(img, 3 * ROUNDS * PIECE, bulk_send.at[1], img_recv.at[0]).wait_send()
    all_of(cap, TILES * ROWS, bulk_send.at[2], core_recv.at[0]).wait_send()
    for out in exchanged([(meta, 15, 0), (table, 7, 1)]) + outs:
        out.wait_send()
    for result in results:
        result.wait()

    for out in outs2:
        out.wait_recv()
    total = jnp.sum(part_a[...], axis=0) + jnp.sum(part_b[...], axis=0)
    loss_out[0:1, :] = jnp.broadcast_to(
        jnp.sum(total, axis=1, keepdims=True) * LN2 / (2.0 * real), (1, 128)
    )
    for out in outs2:
        out.wait_send()


def local(captions, images, positives, valid):
    f32, i32 = jnp.float32, jnp.int32
    dma = pltpu.SemaphoreType.DMA
    vmem = pl.BlockSpec(memory_space=pltpu.VMEM)
    hbm = pl.BlockSpec(memory_space=pl.ANY)
    cap_loss, img_loss, loss = pl.pallas_call(
        kernel,
        out_shape=(
            jax.ShapeDtypeStruct((ROWS,), f32),
            jax.ShapeDtypeStruct((ROWS,), f32),
            jax.ShapeDtypeStruct((1, 128), f32),
        ),
        in_specs=[hbm, hbm, vmem, vmem],
        out_specs=(hbm, hbm, vmem),
        scratch_shapes=[
            pltpu.VMEM((TILES * TILE, WIDTH), jnp.bfloat16),
            pltpu.VMEM((BLOCKS * BLOCK, WIDTH), jnp.bfloat16),
            *[pltpu.VMEM((TILE, BLOCK), f32)] * 4,
            pltpu.VMEM((TILES * TILE, 128), f32),
            pltpu.VMEM((TILES * TILE, 128), f32),
            pltpu.VMEM((BLOCKS, TILES * TILE, 128), f32),
            pltpu.VMEM((BLOCKS, TILES * TILE, 128), f32),
            pltpu.VMEM((TILES * TILE, 128), f32),
            pltpu.VMEM((TILES, 8, BLOCKS * BLOCK), f32),
            pltpu.VMEM((TILES, 8, BLOCKS * BLOCK), f32),
            pltpu.VMEM((TILES, 8, BLOCKS * BLOCK), f32),
            pltpu.VMEM((1, BLOCKS * BLOCK), f32),
            pltpu.VMEM((1, BLOCKS * BLOCK), f32),
            pltpu.VMEM((16, 2, 128), i32),
            pltpu.VMEM((8, 1, 128), i32),
            pltpu.VMEM((24, 128), f32),
            pltpu.VMEM((16, 128), f32),
            pltpu.VMEM((16, 24, 128), f32),
            pltpu.VMEM((16, 3, 128), f32),
            pltpu.VMEM((16, 3, 128), f32),
            pltpu.VMEM((24, 128), f32),
            pltpu.VMEM((8, 16, 128), f32),
            pltpu.VMEM((8, 2, 128), f32),
            pltpu.VMEM((8, 2, 128), f32),
            pltpu.VMEM((16, 128), f32),
            pltpu.VMEM((16, 1, 128), f32),
            pltpu.VMEM((8, 1, 128), f32),
            pltpu.VMEM((ROWS,), f32),
            pltpu.VMEM((ROWS,), f32),
            dma((2,)), dma((2,)), dma((3,)), dma((ROUNDS,)), dma((ROUNDS,)), dma((TILES,)), dma((8,)), dma((8,)),
        ],
        compiler_params=pltpu.CompilerParams(
            collective_id=0, has_side_effects=True, vmem_limit_bytes=62 * 1024 * 1024
        ),
    )(captions, images, positives.reshape(1, ROWS), valid.reshape(1, ROWS))
    return cap_loss, img_loss, loss[0, 0]


def solution(mesh):
    torus = Mesh(mesh.devices.reshape(4, 2, 4, 2, mesh.shape["rep"]), AXES)
    return jax.shard_map(
        local,
        mesh=torus,
        in_specs=(P(AXES, None), P(AXES, None), P(AXES), P(AXES)),
        out_specs=(P(AXES), P(AXES), P()),
        check_vma=False,
    )
```

```python
import functools

import jax
import jax.numpy as jnp
from jax import lax
from jax.experimental import pallas as pl
from jax.experimental.pallas import tpu as pltpu
from jax.sharding import Mesh
from jax.sharding import PartitionSpec as P

AXES = ("blk_0", "blk_1", "blk_2", "blk_3", "rep")
MESH = pl.DeviceIdType.MESH

ROWS = 192
PIECE = 64
WIDTH = 768
TILE = 2 * ROWS
BLOCK = 256
TILES = 8
BLOCKS = 6
LOW = -1e30
LOG2E = 1.4426950408889634
LN2 = 0.6931471805599453

FROM_LEFT = ((3, 0, 0), (3, 0, 1), (3, 0, 2), (2, 0, 0), (2, 0, 1), (3, 1, 2), (2, 1, 1))
FROM_RIGHT = ((1, 0, 0), (1, 0, 1), (1, 0, 2), (1, 1, 0), (2, 0, 2), (1, 1, 1), (2, 1, 0))
FROM_SIDE = ((0, 1, 0), (0, 1, 1), (0, 1, 2), (3, 1, 0), (3, 1, 1), (1, 1, 2), (2, 1, 2))
ARRIVALS = (FROM_LEFT, FROM_RIGHT, FROM_SIDE)
ROUNDS = 7
SLOT = {(0, 0, t): t for t in range(3)}
for _link, _list in enumerate(ARRIVALS):
    for _r, _chunk in enumerate(_list):
        SLOT[_chunk] = 3 * (_r + 1) + _link


RIGHT = {k for (_, _, t), k in SLOT.items() if t == 1}


def sent(link, r):
    d, s, t = ARRIVALS[link][r]
    if link == 0:
        return SLOT[((d + 1) % 4, s, t)]
    if link == 1:
        return SLOT[((d + 3) % 4, s, t)]
    return SLOT[(d, 1 - s, t)]


def release(link, r):
    return max(sent(link, k) // 3 for k in range(r + 1))


def items():
    done, order, starts, pairs = set(), [], {}, {}
    ready = (1, 2, 3, 5, 6, 7)
    for r in range(1, ROUNDS + 1):
        blocks = [b for b in range(BLOCKS) if ready[b] <= r]
        new = [b for b in blocks if ready[b] == r]
        first = [(p, b) for b in new for p in range(r)]
        later = [(r, b) for b in blocks]
        fresh = [i for i in first + later if i not in done]
        starts[r] = len(order)
        pairs[r] = len(order) + len([i for i in first if i not in done])
        order += fresh
        done |= set(fresh)
    return order, starts, pairs


ORDER, STARTS, PAIRS_AT = items()
ITEMS = len(ORDER)
GROUP = 2
STEPS = ITEMS // GROUP
EARLY = 2
AT_STEP = {3: 1, 4: 4, 5: 7, 6: 11, 7: 16}
CORE_AT_STEP = {r: max(PAIRS_AT[r] // GROUP, 1) for r in STARTS}


def segments():
    found = []
    for i, (p, b) in enumerate(ORDER):
        if found:
            k, p0, b0, dp, db, n = found[-1]
            if n == 1:
                step = (p - p0, b - b0)
                if step in ((0, 1), (1, 0)):
                    found[-1] = (k, p0, b0, *step, 2)
                    continue
            elif (p0 + dp * n, b0 + db * n) == (p, b):
                found[-1] = (k, p0, b0, dp, db, n + 1)
                continue
        found.append((i, p, b, 0, 0, 1))
    return found


SEGMENTS = segments()


def place(i):
    tile, block = jnp.int32(0), jnp.int32(0)
    for k, p0, b0, dp, db, _ in SEGMENTS:
        tile = jnp.where(i >= k, p0 + dp * (i - k), tile)
        block = jnp.where(i >= k, b0 + db * (i - k), block)
    return tile, block


def row_place(slot, core):
    return (slot // 3) * TILE + core * ROWS + (slot % 3) * PIECE


def kernel(
    cap_in, img_in, pos_in, valid_in,
    cap_out, img_out, loss_out,
    cap, img, score0, score1, score2, score3, key, row_bias, row_max, row_sum, row_match,
    col_max, col_sum, col_match, col_bias, col_id,
    meta, table, cap_ok, img_ok, row_all, row_msg, row_got, row_lse, col_all, col_msg, col_got, col_lse,
    part_a, part_b, cap_res, img_res,
    load_sem, out_sem, bulk_send, cap_recv, img_recv, core_recv, small_send, small_recv,
):
    x, yh, z, c, yl = (lax.axis_index(a) for a in AXES)
    scores = (score0, score1, score2, score3)

    def group_a(d, s, o):
        return (lax.rem(x + d, 4), yh, z, lax.rem(c + o, 2), lax.rem(yl + s, 2))

    def group_b(d, s):
        return (x, lax.rem(yh + s, 2), lax.rem(z + d, 4), c, lax.rem(yl + s, 2))

    members_a = [(d, s, o) for d in range(4) for s in range(2) for o in range(2) if (d, s, o) != (0, 0, 0)]
    members_b = [(d, s) for d in range(4) for s in range(2) if (d, s) != (0, 0)]
    members_a.sort(key=lambda m: -(2 * min(m[0], 4 - m[0]) + 2 * m[1] + m[2]))
    members_b.sort(key=lambda m: -(min(m[0], 4 - m[0]) + m[1]))

    def copy(src, dst, ssem, rsem, target):
        return pltpu.make_async_remote_copy(
            src_ref=src, dst_ref=dst, send_sem=ssem, recv_sem=rsem, device_id=target, device_id_type=MESH
        )

    def place_a(d, s, o):
        return (d * 2 + s) * 2 + o

    def place_b(d, s):
        return d * 2 + s

    load_cap = pltpu.make_async_copy(cap_in, cap.at[pl.ds(0, ROWS)], load_sem.at[0])
    load_img = pltpu.make_async_copy(img_in, img.at[pl.ds(0, ROWS)], load_sem.at[1])
    load_cap.start()
    load_img.start()

    barrier = pltpu.get_barrier_semaphore()
    for m in members_a:
        pl.semaphore_signal(barrier, inc=1, device_id=group_a(*m), device_id_type=MESH)
    for m in members_b:
        pl.semaphore_signal(barrier, inc=1, device_id=group_b(*m), device_id_type=MESH)

    lane = lax.broadcasted_iota(jnp.int32, (1, 128), 1)
    low_half = lane < 64
    pos_lo = pos_in[0:1, 0:128]
    pos_hi = jnp.concatenate([pos_in[0:1, 128:192], jnp.zeros((1, 64), jnp.int32)], axis=1)
    ok_lo = valid_in[0:1, 0:128]
    ok_hi = jnp.concatenate([valid_in[0:1, 128:192], jnp.zeros((1, 64), jnp.int32)], axis=1)
    meta[0, 0:1, :] = pos_lo + pos_hi * 32768
    meta[0, 1:2, :] = ok_lo + ok_hi * 2

    row_match[...] = jnp.zeros_like(row_match)
    row_sum[...] = jnp.zeros_like(row_sum)
    row_max[...] = jnp.full_like(row_max, 2 * LOW)

    pl.semaphore_wait(barrier, len(members_a) + len(members_b))

    for d, s, o in members_a:
        there = place_a((4 - d) % 4, s, o)
        copy(meta.at[0], meta.at[there], small_send.at[0], small_recv.at[0], group_a(d, s, o)).start()

    ring_a = (group_a(1, 0, 0), group_a(3, 0, 0), group_a(0, 1, 0))
    ring_b = (group_b(1, 0), group_b(3, 0), group_b(0, 1))
    other = group_a(0, 0, 1)

    def cap_copy(link, r):
        src, dst = row_place(sent(link, r), 0), row_place(3 * (r + 1) + link, 0)
        return copy(
            cap.at[pl.ds(src, PIECE)], cap.at[pl.ds(dst, PIECE)],
            bulk_send.at[0], cap_recv.at[r], ring_a[link],
        )

    def img_copy(link, r):
        src, dst = sent(link, r) * PIECE, (3 * (r + 1) + link) * PIECE
        return copy(
            img.at[pl.ds(src, PIECE)], img.at[pl.ds(dst, PIECE)],
            bulk_send.at[1], img_recv.at[r], ring_b[link],
        )

    def core_copy(r):
        return copy(
            cap.at[pl.ds(r * TILE, ROWS)], cap.at[pl.ds(r * TILE + ROWS, ROWS)],
            bulk_send.at[2], core_recv.at[r], other,
        )

    def all_of(ref, count, send, recv):
        part = ref.at[pl.ds(0, count)]
        return copy(part, part, send, recv, other)

    def forward(after, which=(0, 1)):
        for r in range(ROUNDS):
            for link in range(3):
                if release(link, r) == after:
                    if 0 in which:
                        cap_copy(link, r).start()
                    if 1 in which:
                        img_copy(link, r).start()

    def arrive(r):
        all_of(cap, ROWS, bulk_send.at[0], cap_recv.at[r - 1]).wait_recv()
        core_copy(r).start()
        all_of(img, ROWS, bulk_send.at[1], img_recv.at[r - 1]).wait_recv()
        forward(r)

    def arrive_core(r):
        core_copy(r).wait_recv()

    load_cap.wait()
    load_img.wait()
    for r in range(3):
        for link in range(3):
            cap_copy(link, r).start()
            if r < 2:
                img_copy(link, r).start()
    core_copy(0).start()

    all_of(meta, 15, small_send.at[0], small_recv.at[0]).wait_recv()

    word = jnp.zeros((1, 128), jnp.int32)
    for d in range(4):
        for s in range(2):
            for o in range(2):
                at = lax.rem(x + d, 4) * 4 + lax.rem(c + o, 2) * 2 + lax.rem(yl + s, 2)
                word = word | lax.shift_left(
                    meta[place_a(d, s, o), 1:2, :], jnp.broadcast_to(2 * at, (1, 128))
                )
    mine = yh * 4 + z
    table[mine] = word
    for d, s in members_b:
        copy(table.at[mine], table.at[mine], small_send.at[1], small_recv.at[1], group_b(d, s)).start()
    for link in range(3):
        img_copy(link, 2).start()

    def multiply(i, into):
        tile, block = place(i)
        rows = pl.ds(pl.multiple_of(tile * TILE, TILE), TILE)
        cols = pl.ds(pl.multiple_of(block * BLOCK, BLOCK), BLOCK)
        into[...] = lax.dot_general(
            cap[rows, :], img[cols, :], (((1,), (1,)), ((), ())), preferred_element_type=jnp.float32
        )

    for r in range(1, EARLY + 1):
        arrive(r)
    arrive_core(0)
    arrive_core(1)
    for k in range(GROUP):
        multiply(jnp.int32(k), scores[k])

    all_of(table, 7, small_send.at[1], small_recv.at[1]).wait_recv()

    for d in range(4):
        for s in range(2):
            ph, pz, pc = lax.rem(yh + s, 2), lax.rem(z + d, 4), lax.rem(yl + s, 2)
            base = (pz * 2 + pc) * 2
            for half in range(2):
                shift = 2 * (x * 4 + c * 2 + pc) + half
                bits = lax.shift_right_logical(table[ph * 4 + pz], jnp.broadcast_to(shift, (1, 128))) & 1
                img_ok[pl.ds(base + half, 1), :] = bits.astype(jnp.float32)

    for pair in range(12):
        ids, flags = [], []
        for half in range(2):
            slot = 2 * pair + half
            d, s, t = next(k for k, v in SLOT.items() if v == slot)
            ph, pz, pc = lax.rem(yh + s, 2), lax.rem(z + d, 4), lax.rem(yl + s, 2)
            device = (((x * 2 + ph) * 4 + pz) * 2 + c) * 2 + pc
            shift = 2 * (x * 4 + c * 2 + pc) + (1 if t == 2 else 0)
            bits = lax.shift_right_logical(table[ph * 4 + pz], jnp.broadcast_to(shift, (1, 128))) & 1
            if (t == 1) != (half == 1):
                bits = pltpu.roll(bits, 64, 1)
            flags.append(bits)
            ids.append(device * ROWS + t * PIECE - half * 64 + lane)
        flag = jnp.where(low_half, flags[0], flags[1])
        col_bias[0:1, pair * 128 : (pair + 1) * 128] = jnp.where(flag > 0, 0.0, LOW)
        col_id[0:1, pair * 128 : (pair + 1) * 128] = jnp.where(low_half, ids[0], ids[1]).astype(jnp.float32)

    words = jnp.concatenate([table[b] for b in range(8)], axis=0)
    bytes_ = jnp.concatenate(
        [(lax.shift_right_logical(words, jnp.full((8, 128), 8 * q, jnp.int32)) & 255) for q in range(4)], axis=0
    ).astype(jnp.float32).astype(jnp.bfloat16)
    sub = lax.broadcasted_iota(jnp.int32, (128, 128), 0)
    sub8 = lax.broadcasted_iota(jnp.int32, (8, 128), 0)

    def look_up(p):
        pick = ((p >> 6) * 171) >> 9
        row = p - pick * ROWS
        high = (row >= 128).astype(jnp.int32)
        at = row - 128 * high
        here = (((pick >> 4) & 1) << 2) + ((pick >> 2) & 3)
        bit = ((((pick >> 5) << 2) + (pick & 3)) << 1) + high
        hot = (sub == at).astype(jnp.float32).astype(jnp.bfloat16)
        got = jnp.dot(bytes_, hot, preferred_element_type=jnp.float32).astype(jnp.int32)
        value = jnp.zeros((1, 128), jnp.int32)
        for q in range(4):
            mine_q = jnp.sum(jnp.where(sub8 == here, got[8 * q : 8 * q + 8], 0), axis=0, keepdims=True)
            value = jnp.where((bit >> 3) == q, mine_q, value)
        return lax.shift_right_logical(value, bit & 7) & 1

    for d in range(4):
        for s in range(2):
            base = (lax.rem(x + d, 4) * 2 + lax.rem(yl + s, 2)) * 3
            last = jnp.zeros((1, 128), jnp.float32)
            for o in range(2):
                packed = meta[place_a(d, s, o), 0:1, :]
                core = lax.rem(c + o, 2)
                for half in range(2):
                    p = (packed & 32767) if half == 0 else (packed >> 15)
                    ok = look_up(p)
                    real = ok.astype(jnp.float32)
                    if half == 0:
                        cap_ok[pl.ds(base + core, 1), :] = real
                    else:
                        real = jnp.where(low_half, real, 0.0)
                        last = last + jnp.where(core == 1, pltpu.roll(real, 64, 1), real)
                        if o == 1:
                            cap_ok[pl.ds(base + 2, 1), :] = last
                    wanted = jnp.where(ok > 0, p, -1).astype(jnp.float32)
                    turned = jnp.transpose(jnp.broadcast_to(wanted, (128, 128)))
                    for t in (0, 1) if half == 0 else (2,):
                        rows = pl.ds(row_place(SLOT[(d, s, t)], o), PIECE)
                        value = turned[64 * (t % 2) : 64 * (t % 2) + 64]
                        key[rows, :] = value
                        row_bias[rows, :] = jnp.where(value < 0, LOW, 0.0)

    arrive_core(2)

    def peaks(i, held):
        tile, block = place(i)
        first = pl.multiple_of(tile * TILE, TILE)
        cols = [pl.ds(pl.multiple_of(block * BLOCK, BLOCK) + 128 * h, 128) for h in range(2)]
        bias = [jnp.broadcast_to(col_bias[0:1, cols[h]], (PIECE, 128)) for h in range(2)]
        peak = [None, None]
        for k in range(TILE // PIECE):
            rows = pl.ds(first + k * PIECE, PIECE)
            here = pl.ds(k * PIECE, PIECE)
            low = row_bias[rows, :]
            values = []
            for h in range(2):
                u = held[here, 128 * h : 128 * h + 128] * LOG2E + bias[h] + low
                held[here, 128 * h : 128 * h + 128] = u
                top = jnp.max(u.reshape(PIECE // 8, 8, 128), axis=0)
                peak[h] = top if peak[h] is None else jnp.maximum(peak[h], top)
                values.append(u)
            old = row_max[rows, :]
            high = jnp.maximum(jnp.max(jnp.maximum(values[0], values[1]), axis=1, keepdims=True), old)
            row_sum[rows, :] = row_sum[rows, :] * jnp.exp2(old - high)
            row_max[rows, :] = high
        return peak

    def sums(i, held, peak):
        tile, block = place(i)
        first = pl.multiple_of(tile * TILE, TILE)
        cols = [pl.ds(pl.multiple_of(block * BLOCK, BLOCK) + 128 * h, 128) for h in range(2)]
        ids = [jnp.broadcast_to(col_id[0:1, cols[h]], (PIECE, 128)) for h in range(2)]
        total = [jnp.zeros((8, 128), jnp.float32) for _ in range(2)]
        match = [jnp.zeros((8, 128), jnp.float32) for _ in range(2)]
        for k in range(TILE // PIECE):
            rows = pl.ds(first + k * PIECE, PIECE)
            here = pl.ds(k * PIECE, PIECE)
            high = row_max[rows, :]
            wanted = key[rows, :]
            found = row_match[rows, :]
            row_total = row_sum[rows, :]
            for h in range(2):
                u = held[here, 128 * h : 128 * h + 128]
                e = jnp.exp2(u - high)
                row_total = row_total + e
                hit = wanted == ids[h]
                found = jnp.where(hit, u, found)
                for g in range(PIECE // 8):
                    part_u = u[8 * g : 8 * g + 8]
                    total[h] = total[h] + jnp.exp2(part_u - peak[h])
                    match[h] = jnp.where(hit[8 * g : 8 * g + 8], part_u, match[h])
            row_sum[rows, :] = row_total
            row_match[rows, :] = found
        for h in range(2):
            col_max[tile, :, cols[h]] = peak[h]
            col_sum[tile, :, cols[h]] = total[h]
            col_match[tile, :, cols[h]] = match[h]

    def all_statistics(i, held):
        for k in range(0, GROUP, 2):
            tops = [peaks(i + k + j, held[k + j]) for j in range(2)]
            for j in range(2):
                sums(i + k + j, held[k + j], tops[j])

    def advance(step, half):
        for r in range(EARLY + 1, ROUNDS + 1):
            if (AT_STEP[r] - 1) % 2 == half:
                @pl.when(step + 1 == AT_STEP[r])
                def _():
                    arrive(r)
            if (CORE_AT_STEP[r] - 1) % 2 == half:
                @pl.when(step + 1 == CORE_AT_STEP[r])
                def _():
                    arrive_core(r)
        i = GROUP * step
        for k in range(GROUP):
            multiply(i + GROUP + k, scores[(1 - half) * GROUP + k])
        all_statistics(i, scores[half * GROUP :])

    @pl.loop(0, (STEPS - 1) // 2)
    def _(turn):
        for half in range(2):
            advance(turn * 2 + half, half)

    if STEPS % 2 == 0:
        advance(jnp.int32(STEPS - 2), 0)
    all_statistics(jnp.int32(ITEMS - GROUP), scores[((STEPS - 1) % 2) * GROUP :])

    sub64 = lax.broadcasted_iota(jnp.int32, (PIECE, 128), 0)
    lane64 = lax.broadcasted_iota(jnp.int32, (PIECE, 128), 1)

    def row_result(slot, core, shift):
        rows = pl.ds(row_place(slot, core), PIECE)
        high, total = row_max[rows, :], row_sum[rows, :]
        lse = high + jnp.log2(jnp.sum(total, axis=1, keepdims=True))
        found = jnp.sum(row_match[rows, :], axis=1, keepdims=True)
        lse_lane = lane64 == sub64 + shift
        lane_shift = 64 if slot in RIGHT else 0
        found_lane = lane64 == sub64 + lane_shift
        return (
            jnp.sum(jnp.where(lse_lane, lse, 0.0), axis=0, keepdims=True),
            jnp.sum(jnp.where(found_lane, found, 0.0), axis=0, keepdims=True),
        )

    matched = jnp.zeros((1, 128), jnp.float32)
    for d in range(4):
        for s in range(2):
            base = (lax.rem(x + d, 4) * 2 + lax.rem(yl + s, 2)) * 3
            last = jnp.zeros((1, 128), jnp.float32)
            for o in range(2):
                at, core = place_a(d, s, o), lax.rem(c + o, 2)
                first, second = (row_result(SLOT[(d, s, t)], o, 64 * t) for t in range(2))
                third = row_result(SLOT[(d, s, 2)], o, 64 * core)
                row_all[0, pl.ds(base + core, 1), :] = first[0] + second[0]
                last = last + third[0]
                into = row_got if at == 0 else row_msg
                into[at, 0:1, :] = first[1] + second[1]
                into[at, 1:2, :] = third[1]
                matched = matched + first[1] + second[1] + third[1]
            row_all[0, pl.ds(base + 2, 1), :] = last
    row_got[0, 2:3, :] = matched
    for at in range(1, 16):
        row_msg[at, 2:3, :] = matched

    def merged(peak, total):
        high = jnp.max(jnp.max(peak, axis=0), axis=0, keepdims=True)
        total = jnp.sum(total * jnp.exp2(peak - high[None]), axis=0)
        return high + jnp.log2(jnp.sum(total, axis=0, keepdims=True))

    columns = []
    for pair in range(12):
        cols = pl.ds(pair * 128, 128)
        columns.append((
            merged(col_max[:, :, cols], col_sum[:, :, cols]),
            jnp.sum(jnp.sum(col_match[:, :, cols], axis=0), axis=0, keepdims=True),
        ))

    def third_of(slot, which, right):
        value = columns[slot // 2][which]
        return pltpu.roll(value, 64, 1) if (slot % 2 == 1) != right else value

    for d in range(4):
        for s in range(2):
            at = place_b(d, s)
            base = (lax.rem(z + d, 4) * 2 + lax.rem(yl + s, 2)) * 2
            into = col_got if at == 0 else col_msg
            for which in range(2):
                left = third_of(SLOT[(d, s, 0)], which, False)
                right = third_of(SLOT[(d, s, 1)], which, True)
                both = jnp.where(low_half, left, right)
                last = third_of(SLOT[(d, s, 2)], which, False)
                if which == 0:
                    col_all[0, pl.ds(base, 1), :] = both
                    col_all[0, pl.ds(base + 1, 1), :] = last
                else:
                    into[at, 0:1, :] = both
                    into[at, 1:2, :] = last

    def exchange(members, index, target, pairs):
        for m in members:
            here, there = index(*m), index((4 - m[0]) % 4, *m[1:])
            for src, dst, k in pairs:
                copy(src(here), dst.at[there], small_send.at[k], small_recv.at[k], target(*m)).start()

    def exchanged(refs):
        return [all_of(ref, count, small_send.at[k], small_recv.at[k]) for ref, count, k in refs]

    exchange(members_a, place_a, group_a, [
        (lambda here: row_all.at[0], row_all, 2), (lambda here: row_msg.at[here], row_got, 3),
    ])
    exchange(members_b, place_b, group_b, [
        (lambda here: col_all.at[0], col_all, 4), (lambda here: col_msg.at[here], col_got, 5),
    ])
    outs = exchanged([(row_all, 15, 2), (row_got, 15, 3), (col_all, 7, 4), (col_got, 7, 5)])
    for out in outs:
        out.wait_recv()

    def joined(values):
        high = jnp.max(values, axis=0)
        return high + jnp.log2(jnp.sum(jnp.exp2(values - high[None]), axis=0))

    row_lse[...] = joined(row_all[...])
    col_lse[...] = joined(col_all[...])
    row_part = jnp.sum(jnp.where(cap_ok[...] > 0, row_lse[...], 0.0), axis=0, keepdims=True)
    found = jnp.sum(row_got[...], axis=0)
    part_b[0] = row_part - 2.0 * found[2:3]
    odd = lax.broadcasted_iota(jnp.int32, (16, 128), 0) & 1
    wide = lax.broadcasted_iota(jnp.int32, (16, 128), 1)
    counted = (img_ok[...] > 0) & ((odd == 0) | (wide < 64))
    part_a[0] = jnp.sum(jnp.where(counted, col_lse[...], 0.0), axis=0, keepdims=True)
    exchange(members_a, place_a, group_a, [(lambda here: part_a.at[0], part_a, 6)])
    exchange(members_b, place_b, group_b, [(lambda here: part_b.at[0], part_b, 7)])
    outs2 = exchanged([(part_a, 15, 6), (part_b, 7, 7)])

    base = (x * 2 + yl) * 3
    cap_lo = row_lse[pl.ds(base + c, 1), :] - found[0:1]
    cap_hi = row_lse[pl.ds(base + 2, 1), :]
    cap_hi = jnp.where(c == 1, pltpu.roll(cap_hi, 64, 1), cap_hi) - found[1:2]
    real_hi = cap_ok[pl.ds(base + 2, 1), :]
    real_hi = jnp.where(c == 1, pltpu.roll(real_hi, 64, 1), real_hi)
    cap_res[0:128] = jnp.where(cap_ok[pl.ds(base + c, 1), :] > 0, cap_lo * LN2, 0.0).reshape(128)
    cap_res[128:192] = jnp.where(real_hi > 0, cap_hi * LN2, 0.0)[:, 0:64].reshape(64)
    base = (z * 2 + yl) * 2
    found = jnp.sum(col_got[...], axis=0)
    img_lo = col_lse[pl.ds(base, 1), :] - found[0:1]
    img_hi = col_lse[pl.ds(base + 1, 1), :] - found[1:2]
    img_res[0:128] = jnp.where(ok_lo > 0, img_lo * LN2, 0.0).reshape(128)
    img_res[128:192] = jnp.where(ok_hi > 0, img_hi * LN2, 0.0)[:, 0:64].reshape(64)
    results = [
        pltpu.make_async_copy(cap_res, cap_out, out_sem.at[0]), pltpu.make_async_copy(img_res, img_out, out_sem.at[1])
    ]
    for result in results:
        result.start()
    count = jnp.zeros((8, 128), jnp.int32)
    for b in range(32):
        count = count + (lax.shift_right_logical(words, jnp.full((8, 128), b, jnp.int32)) & 1)
    real = jnp.sum(jnp.sum(count, axis=0, keepdims=True).astype(jnp.float32), axis=1, keepdims=True)

    all_of(cap, 3 * ROUNDS * PIECE, bulk_send.at[0], cap_recv.at[0]).wait_send()
    all_of(img, 3 * ROUNDS * PIECE, bulk_send.at[1], img_recv.at[0]).wait_send()
    all_of(cap, TILES * ROWS, bulk_send.at[2], core_recv.at[0]).wait_send()
    for out in exchanged([(meta, 15, 0), (table, 7, 1)]) + outs:
        out.wait_send()
    for result in results:
        result.wait()

    for out in outs2:
        out.wait_recv()
    total = jnp.sum(part_a[...], axis=0) + jnp.sum(part_b[...], axis=0)
    loss_out[0:1, :] = jnp.broadcast_to(
        jnp.sum(total, axis=1, keepdims=True) * LN2 / (2.0 * real), (1, 128)
    )
    for out in outs2:
        out.wait_send()


def local(captions, images, positives, valid):
    f32, i32 = jnp.float32, jnp.int32
    dma = pltpu.SemaphoreType.DMA
    vmem = pl.BlockSpec(memory_space=pltpu.VMEM)
    hbm = pl.BlockSpec(memory_space=pl.ANY)
    cap_loss, img_loss, loss = pl.pallas_call(
        kernel,
        out_shape=(
            jax.ShapeDtypeStruct((ROWS,), f32),
            jax.ShapeDtypeStruct((ROWS,), f32),
            jax.ShapeDtypeStruct((1, 128), f32),
        ),
        in_specs=[hbm, hbm, vmem, vmem],
        out_specs=(hbm, hbm, vmem),
        scratch_shapes=[
            pltpu.VMEM((TILES * TILE, WIDTH), jnp.bfloat16),
            pltpu.VMEM((BLOCKS * BLOCK, WIDTH), jnp.bfloat16),
            *[pltpu.VMEM((TILE, BLOCK), f32)] * 4,
            pltpu.VMEM((TILES * TILE, 128), f32),
            pltpu.VMEM((TILES * TILE, 128), f32),
            pltpu.VMEM((TILES * TILE, 128), f32),
            pltpu.VMEM((TILES * TILE, 128), f32),
            pltpu.VMEM((TILES * TILE, 128), f32),
            pltpu.VMEM((TILES, 8, BLOCKS * BLOCK), f32),
            pltpu.VMEM((TILES, 8, BLOCKS * BLOCK), f32),
            pltpu.VMEM((TILES, 8, BLOCKS * BLOCK), f32),
            pltpu.VMEM((1, BLOCKS * BLOCK), f32),
            pltpu.VMEM((1, BLOCKS * BLOCK), f32),
            pltpu.VMEM((16, 2, 128), i32),
            pltpu.VMEM((8, 1, 128), i32),
            pltpu.VMEM((24, 128), f32),
            pltpu.VMEM((16, 128), f32),
            pltpu.VMEM((16, 24, 128), f32),
            pltpu.VMEM((16, 3, 128), f32),
            pltpu.VMEM((16, 3, 128), f32),
            pltpu.VMEM((24, 128), f32),
            pltpu.VMEM((8, 16, 128), f32),
            pltpu.VMEM((8, 2, 128), f32),
            pltpu.VMEM((8, 2, 128), f32),
            pltpu.VMEM((16, 128), f32),
            pltpu.VMEM((16, 1, 128), f32),
            pltpu.VMEM((8, 1, 128), f32),
            pltpu.VMEM((ROWS,), f32),
            pltpu.VMEM((ROWS,), f32),
            dma((2,)), dma((2,)), dma((3,)), dma((ROUNDS,)), dma((ROUNDS,)), dma((TILES,)), dma((8,)), dma((8,)),
        ],
        compiler_params=pltpu.CompilerParams(
            collective_id=0, has_side_effects=True, vmem_limit_bytes=62 * 1024 * 1024
        ),
    )(captions, images, positives.reshape(1, ROWS), valid.reshape(1, ROWS))
    return cap_loss, img_loss, loss[0, 0]


def solution(mesh):
    torus = Mesh(mesh.devices.reshape(4, 2, 4, 2, mesh.shape["rep"]), AXES)
    return jax.shard_map(
        local,
        mesh=torus,
        in_specs=(P(AXES, None), P(AXES, None), P(AXES), P(AXES)),
        out_specs=(P(AXES), P(AXES), P()),
        check_vma=False,
    )
```
